512 devices in a mesh: blk: 64 (over y, z), tok: 8 (over x, core).
Axes of the slice: x: 4, y: 8, z: 8, core: 2. Of those that a mesh axis runs over, the one named last changes fastest.
Arguments:
- tokens: bfloat16 [8192, 9216], P(('tok', 'blk')), parts along dimension 0, may hold values from -6 to 6
- block_ids: int32 [8192, 8], P(('tok', 'blk')), parts along dimension 0, may hold values from 0 to 63, all different within a row; in each aligned block of 16 rows (0 to 15, 16 to 31, ...) at most 5 rows name the same one
- w_in: bfloat16 [9216, 8192], P(None, 'blk'), may hold values from -0.0625 to 0.0625
- bias_in: float32 [8192], P('blk'), may hold values from -3 to 3
- w_out: bfloat16 [8192, 9216], P('blk'), may hold values from -0.1875 to 0.1875
Outputs:
- ffn_out: bfloat16 [8192, 9216], P(('tok', 'blk')), parts along dimension 0
The draws below stay inside these ranges and needn't reach their ends.
There are 8 independent parts, one for each index of `tok`. The reference program is written for one: setup_inputs(seed, part) draws one part's arguments, and reference() takes and returns one part's arrays. A program takes and returns all parts, laid end to end along the dimension named above; an argument that names none is the same for every part. Nothing has to cross between parts.
Inputs may be any that keep to these rules, and one draw needn't show every extreme that they name: `block_ids`: each row names 8 different blocks. Among the 16 rows of one device no block is named by more than 5 rows, and some block is named by exactly 5 of them.
All inputs are finite; a program needn't handle non-finite values.
Results may differ from the reference program's by a relative error of at most 0.0057.
Values may be sent and summed in bfloat16 or wider, within the bound.
No kernel may reach another device: no remote copies, remote signals or barrier semaphores. Data moves between devices by JAX's collectives and lax.ppermute only.
A program may use at most 128 MiB of HBM per device.

```python
import math
import jax
import jax.numpy as jnp
import numpy as np
from jax import lax

D = 9216
BLOCK = 128
TOK_DEV = 16
BLOCKS = 64
TOPK = 8
CAP = 5
TOKENS = 1024


def levels(key, extent, cuts, least, largest):
    level = 1.0
    for position, parts in cuts:
        draws = jax.random.uniform(jax.random.fold_in(jax.random.fold_in(key, 6), position), (parts,), jnp.float32, least / len(cuts), largest / len(cuts))
        level = level * jnp.repeat(jnp.exp(draws), extent[position] // parts).reshape((-1,) + (1,) * (len(extent) - 1 - position))
    return level


def assign_block(rng, own, number, rows, number_of, top, limit, slope):
    ranking = jax.random.permutation(rng, number_of)
    heavy_load, ordinary = shares(number_of, rows * top, limit, slope, True), shares(number_of, rows * top, limit, slope, False)
    places = jnp.arange(number_of)

    def named(lengths, turn):
        used = int((lengths > 0).sum())
        fixed = max(1, used // 4)
        passed = fixed + (places - fixed + turn * (used - fixed)) % max(1, number_of - fixed)
        return jnp.zeros((number_of,), jnp.int32).at[ranking[jnp.where(places < fixed, places, passed)]].set(jnp.asarray(lengths, jnp.int32))

    lengths = jnp.where(number % 4 == 0, named(heavy_load, number // 4), named(ordinary, number - number // 4 - 1))
    mixed = jax.random.permutation(jax.random.fold_in(own, 3), number_of)
    giver, taker = mixed[0:number_of // 2 * 2:2], mixed[1:number_of // 2 * 2:2]
    slack = jnp.minimum(lengths[giver] - 1, limit - lengths[taker]) // 2
    slack = jnp.where((giver == ranking[0]) | (taker == ranking[0]) | (lengths[taker] == 0), 0, jnp.maximum(slack, 0))
    passed = jax.random.randint(jax.random.fold_in(own, 4), (number_of // 2,), 0, 1 << 20) % (slack + 1)
    lengths = lengths.at[giver].add(-passed).at[taker].add(passed)
    members = jnp.searchsorted(jnp.cumsum(lengths), jnp.arange(rows * top), side="right").astype(jnp.int32)
    listing = members.reshape(top, rows).T
    listing = listing[jax.random.permutation(jax.random.fold_in(own, 1), rows)]
    turn = jax.random.randint(jax.random.fold_in(own, 2), (rows, 1), 0, top)
    return jnp.take_along_axis(listing, (jnp.arange(top)[None, :] + turn) % top, axis=1)


def shares(count, total, bound, skew, full):
    loads = [(1 << 20) // math.isqrt(standing ** skew) + 1 for standing in range(1, count + 1)]
    largest = bound if full else min(bound, max(-(-total // count), total * loads[0] // sum(loads)))
    least = 1 if total - largest >= count - 1 else 0
    counts, rest = [largest] + [least] * (count - 1), total - largest - least * (count - 1)
    while rest > 0:
        movable = [i for i in range(1, count) if counts[i] < largest] or [i for i in range(1, count) if counts[i] < bound]
        pool, budget = sum([loads[i] for i in movable]), rest
        for i in movable:
            more = min(bound - counts[i], max(1, budget * loads[i] // pool), rest)
            counts[i] = counts[i] + more
            rest = rest - more
    return np.array(counts)


def centred(key, shape, width, reach, shards=(), kind=jnp.bfloat16):
    values = width * jax.random.normal(key, shape, jnp.float32)
    if shards:
        values = values * levels(key, shape, shards, -0.22, 0.18)
    return jnp.clip(values, -reach, reach).astype(kind)


def setup_inputs(seed: int = 0, part: int = 0) -> dict:
    keys = jax.random.split(jax.random.key(seed), 6)
    part_keys = jax.random.split(jax.random.fold_in(keys[5], part), 6)
    tokens = centred(part_keys[0], (TOKENS, D), 1.0, 6.0, ((0, 64),))
    block_ids_keys = jax.random.split(jax.random.fold_in(part_keys[1], 1), TOKENS // TOK_DEV)
    block_ids_turns = jax.random.permutation(jax.random.fold_in(part_keys[1], 3), TOKENS // TOK_DEV)
    block_ids = jax.vmap(lambda own, number: assign_block(jax.random.fold_in(part_keys[1], 2), own, number, TOK_DEV, BLOCKS, TOPK, CAP, 2))(block_ids_keys, block_ids_turns).reshape((TOKENS, TOPK))
    w_in = centred(keys[2], (D, BLOCKS * BLOCK), D ** -0.5, 0.0625, ((1, 64),))
    bias_in = centred(keys[3], (BLOCKS * BLOCK,), 0.5, 3.0, ((0, 64),), jnp.float32)
    w_out = centred(keys[4], (BLOCKS * BLOCK, D), (TOPK * BLOCK) ** -0.5, 0.1875, ((0, 64),))
    return {"tokens": tokens, "block_ids": block_ids, "w_in": w_in, "bias_in": bias_in, "w_out": w_out}


def reference(tokens, block_ids, w_in, bias_in, w_out):
    def one_block(total, index):
        start = (index * BLOCK).astype(jnp.int32)
        w_first = lax.dynamic_slice_in_dim(w_in, start, BLOCK, 1)
        b_first = lax.dynamic_slice_in_dim(bias_in, start, BLOCK, 0)
        w_second = lax.dynamic_slice_in_dim(w_out, start, BLOCK, 0)
        pre_act = jnp.dot(tokens, w_first, preferred_element_type=jnp.float32) + b_first.astype(jnp.float32)
        hidden = jnp.maximum(pre_act, 0.0).astype(jnp.bfloat16)
        contrib = jnp.dot(hidden, w_second, preferred_element_type=jnp.float32).astype(jnp.bfloat16).astype(jnp.float32)
        chosen = jnp.any(block_ids == index, axis=1)
        return total + jnp.where(chosen[:, None], contrib, jnp.zeros_like(contrib)), None

    start_total = jnp.zeros((TOKENS, D), jnp.float32)
    total, unused = lax.scan(one_block, start_total, jnp.arange(BLOCKS, dtype=jnp.int32))
    return total.astype(jnp.bfloat16)
```

```python
import functools
import math

import jax
import jax.numpy as jnp
from jax import lax
from jax.experimental import pallas as pl
from jax.experimental.pallas import tpu as pltpu
from jax.sharding import Mesh
from jax.sharding import PartitionSpec as P

CAP = 5
LANES = 128
BF16 = jnp.bfloat16
F32 = jnp.float32


def pack_kernel(where_ref, tokens_ref, ids_ref, w_in_ref, w_out_ref, out_ref, in_rows, sems, *, ny, nt):
    share = where_ref[0]
    width = tokens_ref.shape[1] // ny
    part = width // nt
    toks = tokens_ref.shape[0]
    copies = []
    for k in range(ny):
        copies.append(
            pltpu.make_async_copy(
                w_in_ref.at[pl.ds(k * width + share * part, part), :], in_rows.at[k], sems.at[k]
            )
        )
    for c in copies:
        c.start()
    ids = ids_ref[...]
    lane = lax.broadcasted_iota(jnp.int32, (toks, LANES), 1)
    nz = LANES // 2 // ny
    block = jnp.where(lane < ny * nz, (lane % ny) * nz + lane // ny, -1)
    named = jnp.zeros((toks, LANES), F32)
    for k in range(ids.shape[1]):
        named = jnp.where(ids[:, k : k + 1] == block, 1.0, named)
    row = lax.broadcasted_iota(jnp.int32, (toks, toks), 0)
    col = lax.broadcasted_iota(jnp.int32, (toks, toks), 1)
    before = jnp.where(col < row, 1.0, 0.0).astype(BF16)
    position = jnp.dot(before, named.astype(BF16), preferred_element_type=F32)
    slots = jnp.where(named > 0.0, position, -1.0).astype(BF16)
    for k in range(ny):
        out_ref[k, :, 0:width] = tokens_ref[:, k * width : (k + 1) * width]
        out_ref[k, :, width : width + LANES] = slots
        out_ref[k, :, width + LANES : 2 * width + LANES] = w_out_ref[:, k * width : (k + 1) * width]
    base = 2 * width + LANES
    for k in range(ny):
        copies[k].wait()
        for g in range(part // toks):
            out_ref[k, :, base + g * LANES : base + (g + 1) * LANES] = in_rows[
                k, g * toks : (g + 1) * toks, :
            ]


def pack(where, tokens, ids, w_in, w_out, ny, nt):
    toks, model = tokens.shape
    width = model // ny
    part = width // nt
    return pl.pallas_call(
        functools.partial(pack_kernel, ny=ny, nt=nt),
        out_shape=jax.ShapeDtypeStruct((ny, toks, 3 * width + LANES), BF16),
        grid_spec=pltpu.PrefetchScalarGridSpec(
            num_scalar_prefetch=1,
            grid=(1,),
            in_specs=[
                pl.BlockSpec((toks, model), lambda i, s: (0, 0)),
                pl.BlockSpec(ids.shape, lambda i, s: (0, 0)),
                pl.BlockSpec(memory_space=pl.ANY),
                pl.BlockSpec((w_out.shape[0] // nt, model), lambda i, s: (s[0], 0)),
            ],
            out_specs=pl.BlockSpec((ny, toks, 3 * width + LANES), lambda i, s: (0, 0, 0)),
            scratch_shapes=[
                pltpu.VMEM((ny, part, LANES), BF16),
                pltpu.SemaphoreType.DMA((ny,)),
            ],
        ),
        name="pack",
    )(where, tokens, ids, w_in, w_out)


def first_kernel(x_ref, pick_ref, w_ref, out_ref, wide, *, ny, chunk, toks):
    nt, _, rows, lanes = w_ref.shape
    groups = lanes // LANES
    width = nt * rows * groups
    for t in range(nt):
        for g in range(groups):
            top = (t * groups + g) * rows
            for j in range(ny):
                wide[top : top + rows, j * LANES : (j + 1) * LANES] = w_ref[
                    t, j, :, g * LANES : (g + 1) * LANES
                ]
    per = chunk // toks * CAP
    col = lax.broadcasted_iota(jnp.int32, (pick_ref.shape[0], chunk), 1)
    slot = lax.broadcasted_iota(jnp.int32, (per, chunk), 0).astype(F32)
    first = (col // toks * CAP).astype(F32)
    for m in range(x_ref.shape[0] // chunk):
        x = x_ref[m * chunk : (m + 1) * chunk, 0:width]
        pos = x_ref[m * chunk : (m + 1) * chunk, width : width + LANES]
        h = jnp.dot(x, wide[...], preferred_element_type=F32).astype(BF16)
        at = lax.dot_general(
            pick_ref[...], pos, (((1,), (1,)), ((), ())), preferred_element_type=F32
        )
        at = jnp.where(at >= 0.0, at + first, -1.0)
        for j in range(ny):
            s = jnp.where(slot == at[j : j + 1, :], 1.0, 0.0).astype(BF16)
            rows_j = jnp.dot(s, h[:, j * LANES : (j + 1) * LANES], preferred_element_type=F32)
            out_ref[j, m * per : (m + 1) * per, :] = rows_j.astype(BF16)


def first_product(x, pick, w, ny, toks):
    chunk = 256
    slots = x.shape[0] // toks * CAP
    return pl.pallas_call(
        functools.partial(first_kernel, ny=ny, chunk=chunk, toks=toks),
        out_shape=jax.ShapeDtypeStruct((ny, slots, LANES), BF16),
        scratch_shapes=[pltpu.VMEM((x.shape[1] - LANES, ny * LANES), BF16)],
        name="first_product",
    )(x, pick, w)


def second_kernel(h_ref, pos_ref, pick_ref, w_ref, out_ref, tall, spread, *, ny, chunk, toks):
    nt, _, rows, _ = w_ref.shape
    for j in range(ny):
        for t in range(nt):
            top = (j * nt + t) * rows
            tall[top : top + rows, :] = w_ref[t, j]
    per = chunk // toks * CAP
    row = lax.broadcasted_iota(jnp.int32, (chunk, pick_ref.shape[0]), 0)
    slot = lax.broadcasted_iota(jnp.int32, (chunk, per), 1).astype(F32)
    first = (row // toks * CAP).astype(F32)
    for m in range(pos_ref.shape[0] // chunk):
        pos = pos_ref[m * chunk : (m + 1) * chunk, :]
        at = lax.dot_general(
            pos, pick_ref[...], (((1,), (1,)), ((), ())), preferred_element_type=F32
        )
        at = jnp.where(at >= 0.0, at + first, -1.0)
        for j in range(ny):
            s = jnp.where(slot == at[:, j : j + 1], 1.0, 0.0).astype(BF16)
            full = jnp.dot(s, h_ref[j, m * per : (m + 1) * per, :], preferred_element_type=F32)
            spread[:, j * LANES : (j + 1) * LANES] = full.astype(BF16)
        y = jnp.dot(spread[...], tall[...], preferred_element_type=F32).astype(BF16)
        per_dev = chunk // toks
        out_ref[m * per_dev : (m + 1) * per_dev] = y.reshape(per_dev, toks, y.shape[1])


def second_product(h, x, pick, w, ny, toks):
    chunk = 256
    width = x.shape[1] - LANES
    total = x.shape[0]
    return pl.pallas_call(
        functools.partial(second_kernel, ny=ny, chunk=chunk, toks=toks),
        out_shape=jax.ShapeDtypeStruct((total // toks, toks, width), BF16),
        grid=(1,),
        in_specs=[
            pl.BlockSpec(h.shape, lambda i: (0, 0, 0)),
            pl.BlockSpec((total, LANES), lambda i: (0, width // LANES)),
            pl.BlockSpec(pick.shape, lambda i: (0, 0)),
            pl.BlockSpec(w.shape, lambda i: (0, 0, 0, 0)),
        ],
        out_specs=pl.BlockSpec((total // toks, toks, width), lambda i: (0, 0, 0)),
        scratch_shapes=[
            pltpu.VMEM((ny * LANES, width), BF16),
            pltpu.VMEM((chunk, ny * LANES), BF16),
        ],
        name="second_product",
    )(h, x, pick, w)


def combine_kernel(y_ref, out_ref, *, ny):
    width = y_ref.shape[2]
    for k in range(ny):
        total = y_ref[k].astype(F32)
        for other in range(ny + k, y_ref.shape[0], ny):
            total = total + y_ref[other].astype(F32)
        out_ref[:, k * width : (k + 1) * width] = total.astype(BF16)


def combine(y, ny):
    return pl.pallas_call(
        functools.partial(combine_kernel, ny=ny),
        out_shape=jax.ShapeDtypeStruct((y.shape[1], y.shape[2] * ny), BF16),
        name="combine",
    )(y)


def body(tokens, block_ids, w_in, bias_in, w_out):
    toks = tokens.shape[0]
    ny, nz = lax.axis_size("y"), lax.axis_size("z")
    nt = lax.axis_size("x") * lax.axis_size("c")
    width = tokens.shape[1] // ny
    share = lax.axis_index("x") * lax.axis_size("c") + lax.axis_index("c")
    z = lax.axis_index("z")
    payload = pack(share.reshape(1).astype(jnp.int32), tokens, block_ids, w_in, w_out, ny, nt)
    got = lax.all_to_all(payload, "y", split_axis=0, concat_axis=0, tiled=True)
    x_part = got[:, :, : width + LANES].reshape(ny * toks, width + LANES)
    x = lax.all_gather(x_part, "z", axis=0, tiled=True)
    w1 = got[:, :, 2 * width + LANES :]
    w1 = lax.all_to_all(
        jnp.broadcast_to(w1[None], (nt,) + w1.shape), ("x", "c"), split_axis=0, concat_axis=0, tiled=True
    )
    w2_part = got[:, :, width + LANES : 2 * width + LANES]
    pick = (
        jnp.arange(LANES, dtype=jnp.int32)[None, :] == z * ny + jnp.arange(16, dtype=jnp.int32)[:, None]
    ) & (jnp.arange(16)[:, None] < ny)
    pick = pick.astype(BF16)
    x, w2_part = lax.optimization_barrier((x, w2_part))
    w2 = lax.all_gather(w2_part[None], ("x", "c"), axis=0, tiled=True)
    h = first_product(x, pick, w1, ny, toks)
    h = lax.all_to_all(h, "y", split_axis=0, concat_axis=0, tiled=True)
    h = jnp.sum(h.astype(F32), axis=0) + bias_in[None, :]
    h = jnp.maximum(h, 0.0).astype(BF16)
    h = lax.all_to_all(
        jnp.broadcast_to(h[None], (ny,) + h.shape), "y", split_axis=0, concat_axis=0, tiled=True
    )
    y = second_product(h, x, pick, w2, ny, toks)
    y = lax.all_to_all(y, ("z", "y"), split_axis=0, concat_axis=0, tiled=True)
    return combine(y, ny)


def solution(mesh):
    side = math.isqrt(mesh.shape["blk"])
    cores = 2
    fine = Mesh(
        mesh.devices.reshape(side, side, mesh.shape["tok"] // cores, cores), ("y", "z", "x", "c")
    )
    rows = ("x", "c", "y", "z")
    return jax.shard_map(
        body,
        mesh=fine,
        in_specs=(
            P(rows, None),
            P(rows, None),
            P(None, ("y", "z")),
            P(("y", "z")),
            P(("y", "z"), None),
        ),
        out_specs=P(rows, None),
        check_vma=False,
    )
```

```python
import functools
import math

import jax
import jax.numpy as jnp
from jax import lax
from jax.experimental import pallas as pl
from jax.experimental.pallas import tpu as pltpu
from jax.sharding import Mesh
from jax.sharding import PartitionSpec as P

CAP = 5
LANES = 128
BF16 = jnp.bfloat16
F32 = jnp.float32


def tokens_kernel(tokens_ref, ids_ref, out_ref, *, ny, nz):
    width = tokens_ref.shape[1] // ny
    toks = tokens_ref.shape[0]
    same = lax.broadcasted_iota(jnp.int32, (ids_ref.shape[0],) * 2, 0)
    same = same == lax.broadcasted_iota(jnp.int32, same.shape, 1)
    ids = lax.dot_general(
        ids_ref[...].astype(F32).astype(BF16),
        jnp.where(same, 1.0, 0.0).astype(BF16),
        (((0,), (0,)), ((), ())),
        preferred_element_type=F32,
    )
    lane = lax.broadcasted_iota(jnp.int32, (toks, LANES), 1)
    block = jnp.where(lane < ny * nz, (lane % ny) * nz + lane // ny, -1).astype(F32)
    named = jnp.zeros((toks, LANES), F32)
    for k in range(ids.shape[1]):
        named = jnp.where(ids[:, k : k + 1] == block, 1.0, named)
    row = lax.broadcasted_iota(jnp.int32, (toks, toks), 0)
    col = lax.broadcasted_iota(jnp.int32, (toks, toks), 1)
    before = jnp.where(col < row, 1.0, 0.0).astype(BF16)
    position = jnp.dot(before, named.astype(BF16), preferred_element_type=F32)
    slots = jnp.where(named > 0.0, position, -1.0).astype(BF16)
    for k in range(ny):
        piece = tokens_ref[:, k * width : (k + 1) * width]
        for z in range(nz):
            out_ref[k * nz + z, :, 0:width] = piece
            out_ref[k * nz + z, :, width : width + LANES] = slots


def spread_tokens(tokens, ids, ny, nz):
    toks, model = tokens.shape
    width = model // ny
    return pl.pallas_call(
        functools.partial(tokens_kernel, ny=ny, nz=nz),
        out_shape=jax.ShapeDtypeStruct((ny * nz, toks, width + LANES), BF16),
        name="spread_tokens",
    )(tokens, ids)


def weights_kernel(where_ref, w_in_ref, w_out_ref, out_ref, in_rows, out_rows, sems, *, ny, nt):
    share, y = where_ref[0], where_ref[1]
    width = w_out_ref.shape[1] // ny
    part = width // nt
    rows = out_rows.shape[1]
    copies = []
    for k in range(ny):
        dest = (y + k) % ny
        copies.append(
            pltpu.make_async_copy(
                w_in_ref.at[pl.ds(pl.multiple_of(dest * width + share * part, 16), part), :],
                in_rows.at[k],
                sems.at[k, 0],
            )
        )
        copies.append(
            pltpu.make_async_copy(
                w_out_ref.at[
                    pl.ds(pl.multiple_of(share * rows, 16), rows),
                    pl.ds(pl.multiple_of(dest * width, LANES), width),
                ],
                out_rows.at[k],
                sems.at[k, 1],
            )
        )
    for c in copies:
        c.start()
    for k in range(ny):
        copies[2 * k].wait()
        copies[2 * k + 1].wait()
        out_ref[k, :, 0:width] = out_rows[k]
        for g in range(part // rows):
            out_ref[k, :, width + g * LANES : width + (g + 1) * LANES] = in_rows[
                k, g * rows : (g + 1) * rows, :
            ]


def pack_weights(where, w_in, w_out, ny, nt):
    rows = w_out.shape[0] // nt
    width = w_out.shape[1] // ny
    return pl.pallas_call(
        functools.partial(weights_kernel, ny=ny, nt=nt),
        out_shape=jax.ShapeDtypeStruct((ny, rows, 2 * width), BF16),
        grid_spec=pltpu.PrefetchScalarGridSpec(
            num_scalar_prefetch=1,
            grid=(1,),
            in_specs=[
                pl.BlockSpec(memory_space=pl.ANY),
                pl.BlockSpec(memory_space=pl.ANY),
            ],
            out_specs=pl.BlockSpec((ny, rows, 2 * width), lambda i, s: (0, 0, 0)),
            scratch_shapes=[
                pltpu.VMEM((ny, width // nt, LANES), BF16),
                pltpu.VMEM((ny, rows, width), BF16),
                pltpu.SemaphoreType.DMA((ny, 2)),
            ],
        ),
        name="pack_weights",
    )(where, w_in, w_out)


def tile_kernel(where_ref, mine_ref, other_ref, wide_ref, tall_ref, *, nc):
    x, c = where_ref[2], where_ref[3]
    nx, ny, rows, lanes = mine_ref.shape
    width = lanes // 2
    groups = width // LANES
    for source, core in ((mine_ref, c), (other_ref, nc - 1 - c)):
        for s in range(nx):
            share = (x + nx - s) % nx * nc + core
            for k in range(ny):
                top = pl.multiple_of(k * LANES + share * rows, 16)
                tall_ref[pl.ds(top, rows), :] = source[s, k, :, 0:width]
                for g in range(groups):
                    top = pl.multiple_of((share * groups + g) * rows, 16)
                    wide_ref[pl.ds(top, rows), k * LANES : (k + 1) * LANES] = source[
                        s, k, :, width + g * LANES : width + (g + 1) * LANES
                    ]


def tile_weights(where, mine, other, nc):
    _, ny, _, lanes = mine.shape
    width = lanes // 2
    return pl.pallas_call(
        functools.partial(tile_kernel, nc=nc),
        out_shape=(
            jax.ShapeDtypeStruct((width, ny * LANES), BF16),
            jax.ShapeDtypeStruct((ny * LANES, width), BF16),
        ),
        in_specs=[
            pl.BlockSpec(memory_space=pltpu.SMEM),
            pl.BlockSpec(memory_space=pltpu.VMEM),
            pl.BlockSpec(memory_space=pltpu.VMEM),
        ],
        out_specs=(
            pl.BlockSpec(memory_space=pltpu.VMEM),
            pl.BlockSpec(memory_space=pltpu.VMEM),
        ),
        name="tile_weights",
    )(where, mine, other)


def first_kernel(where_ref, x_ref, pick_ref, wide_ref, out_ref, *, ny, chunk, toks):
    width = wide_ref.shape[0]
    y = where_ref[1]
    per = chunk // toks * CAP
    col = lax.broadcasted_iota(jnp.int32, (pick_ref.shape[0], chunk), 1)
    slot = lax.broadcasted_iota(jnp.int32, (per, chunk), 0).astype(F32)
    first = (col // toks * CAP).astype(F32)
    for m in range(x_ref.shape[0] // chunk):
        x = x_ref[m * chunk : (m + 1) * chunk, 0:width]
        pos = x_ref[m * chunk : (m + 1) * chunk, width : width + LANES]
        h = jnp.dot(x, wide_ref[...], preferred_element_type=F32).astype(BF16)
        at = lax.dot_general(
            pick_ref[...], pos, (((1,), (1,)), ((), ())), preferred_element_type=F32
        )
        at = jnp.where(at >= 0.0, at + first, -1.0)
        for k in range(ny):
            s = jnp.where(slot == at[k : k + 1, :], 1.0, 0.0).astype(BF16)
            rows_k = jnp.dot(s, h[:, k * LANES : (k + 1) * LANES], preferred_element_type=F32)
            out_ref[(y + ny - k) % ny, m * per : (m + 1) * per, :] = rows_k.astype(BF16)


def first_product(where, x, pick, wide, ny, toks):
    chunk = 256
    slots = x.shape[0] // toks * CAP
    return pl.pallas_call(
        functools.partial(first_kernel, ny=ny, chunk=chunk, toks=toks),
        out_shape=jax.ShapeDtypeStruct((ny, slots, LANES), BF16),
        in_specs=[pl.BlockSpec(memory_space=pltpu.SMEM)]
        + [pl.BlockSpec(memory_space=pltpu.VMEM)] * 3,
        out_specs=pl.BlockSpec(memory_space=pltpu.VMEM),
        name="first_product",
    )(where, x, pick, wide)


def second_kernel(where_ref, h_ref, x_ref, pick_ref, tall_ref, out_ref, spread, *, ny, chunk, toks):
    y = where_ref[1]
    width = tall_ref.shape[1]
    per = chunk // toks * CAP
    row = lax.broadcasted_iota(jnp.int32, (chunk, pick_ref.shape[0]), 0)
    slot = lax.broadcasted_iota(jnp.int32, (chunk, per), 1).astype(F32)
    first = (row // toks * CAP).astype(F32)
    for m in range(x_ref.shape[0] // chunk):
        pos = x_ref[m * chunk : (m + 1) * chunk, width : width + LANES]
        at = lax.dot_general(
            pos, pick_ref[...], (((1,), (1,)), ((), ())), preferred_element_type=F32
        )
        at = jnp.where(at >= 0.0, at + first, -1.0)
        for k in range(ny):
            s = jnp.where(slot == at[:, k : k + 1], 1.0, 0.0).astype(BF16)
            full = jnp.dot(
                s, h_ref[(y + ny - k) % ny, m * per : (m + 1) * per, :], preferred_element_type=F32
            )
            spread[:, k * LANES : (k + 1) * LANES] = full.astype(BF16)
        out = jnp.dot(spread[...], tall_ref[...], preferred_element_type=F32).astype(BF16)
        per_dev = chunk // toks
        out_ref[m * per_dev : (m + 1) * per_dev] = out.reshape(per_dev, toks, width)


def second_product(where, h, x, pick, tall, ny, toks):
    chunk = 256
    width = x.shape[1] - LANES
    total = x.shape[0]
    return pl.pallas_call(
        functools.partial(second_kernel, ny=ny, chunk=chunk, toks=toks),
        out_shape=jax.ShapeDtypeStruct((total // toks, toks, width), BF16),
        in_specs=[pl.BlockSpec(memory_space=pltpu.SMEM)]
        + [pl.BlockSpec(memory_space=pltpu.VMEM)] * 4,
        out_specs=pl.BlockSpec(memory_space=pltpu.VMEM),
        scratch_shapes=[pltpu.VMEM((chunk, ny * LANES), BF16)],
        name="second_product",
    )(where, h, x, pick, tall)


def combine_kernel(y_ref, out_ref, *, ny):
    width = y_ref.shape[2]
    for k in range(ny):
        nz = y_ref.shape[0] // ny
        total = y_ref[k * nz].astype(F32)
        for other in range(k * nz + 1, (k + 1) * nz):
            total = total + y_ref[other].astype(F32)
        out_ref[:, k * width : (k + 1) * width] = total.astype(BF16)


def combine(y, ny):
    return pl.pallas_call(
        functools.partial(combine_kernel, ny=ny),
        out_shape=jax.ShapeDtypeStruct((y.shape[1], y.shape[2] * ny), BF16),
        in_specs=[pl.BlockSpec(memory_space=pltpu.VMEM)],
        name="combine",
    )(y)


def steps(n, k):
    return [(i, (i + k) % n) for i in range(n)]


def body(tokens, block_ids, w_in, bias_in, w_out):
    toks = tokens.shape[0]
    ny, nz = lax.axis_size("y"), lax.axis_size("z")
    nx, nc = lax.axis_size("x"), lax.axis_size("c")
    nt = nx * nc
    width = tokens.shape[1] // ny
    y, z = lax.axis_index("y"), lax.axis_index("z")
    place = lax.axis_index("x"), lax.axis_index("c")
    where = jnp.stack([place[0] * nc + place[1], y, place[0], place[1]]).astype(jnp.int32)

    x = spread_tokens(tokens, block_ids.T, ny, nz)
    x, where = lax.optimization_barrier((x, where))
    x = lax.all_to_all(x, ("y", "z"), split_axis=0, concat_axis=0, tiled=True)
    x = x.reshape(-1, width + LANES)

    pieces = pack_weights(where, w_in, w_out, ny, nt)
    got = [pieces[0]]
    for k in range(1, ny):
        got.append(lax.ppermute(pieces[k], "y", steps(ny, k)))
    got = jnp.stack(got)
    mine = [got]
    for s in range(1, nx):
        mine.append(lax.ppermute(got, "x", steps(nx, s)))
    mine = jnp.stack(mine)
    other = lax.ppermute(mine, "c", steps(nc, 1))
    wide, tall = tile_weights(where, mine, other, nc)

    step = jnp.arange(16, dtype=jnp.int32)[:, None]
    lane = jnp.arange(LANES, dtype=jnp.int32)[None, :]
    pick = ((lane == z * ny + (y + ny - step) % ny) & (step < ny)).astype(BF16)
    h = first_product(where, x, pick, wide, ny, toks)
    h = lax.all_to_all(h, "y", split_axis=0, concat_axis=0, tiled=True)
    h = jnp.sum(h.astype(F32), axis=0) + bias_in[None, :]
    h = jnp.maximum(h, 0.0).astype(BF16)
    h = lax.all_to_all(
        jnp.broadcast_to(h[None], (ny,) + h.shape), "y", split_axis=0, concat_axis=0, tiled=True
    )
    out = second_product(where, h, x, pick, tall, ny, toks)
    out = lax.all_to_all(out, ("y", "z"), split_axis=0, concat_axis=0, tiled=True)
    return combine(out, ny)


def solution(mesh):
    side = math.isqrt(mesh.shape["blk"])
    cores = 2
    fine = Mesh(
        mesh.devices.reshape(side, side, mesh.shape["tok"] // cores, cores), ("y", "z", "x", "c")
    )
    rows = ("x", "c", "y", "z")
    return jax.shard_map(
        body,
        mesh=fine,
        in_specs=(
            P(rows, None),
            P(rows, None),
            P(None, ("y", "z")),
            P(("y", "z")),
            P(("y", "z"), None),
        ),
        out_specs=P(rows, None),
        check_vma=False,
    )
```

```python
import functools
import math

import jax
import jax.numpy as jnp
from jax import lax
from jax.experimental import pallas as pl
from jax.experimental.pallas import tpu as pltpu
from jax.sharding import Mesh
from jax.sharding import PartitionSpec as P

CAP = 5
LANES = 128
BF16 = jnp.bfloat16
F32 = jnp.float32


def pack_kernel(where_ref, tokens_ref, ids_ref, w_in_ref, w_out_ref, out_ref, in_rows, sems, *, ny, nz, nt):
    share = where_ref[0]
    width = tokens_ref.shape[1] // ny
    part = width // nt
    toks = tokens_ref.shape[0]
    copies = []
    for k in range(ny):
        copies.append(
            pltpu.make_async_copy(
                w_in_ref.at[pl.ds(k * width + share * part, part), :], in_rows.at[k], sems.at[k]
            )
        )
    for c in copies:
        c.start()
    same = lax.broadcasted_iota(jnp.int32, (ids_ref.shape[0],) * 2, 0)
    same = same == lax.broadcasted_iota(jnp.int32, same.shape, 1)
    ids = lax.dot_general(
        ids_ref[...].astype(F32).astype(BF16),
        jnp.where(same, 1.0, 0.0).astype(BF16),
        (((0,), (0,)), ((), ())),
        preferred_element_type=F32,
    )
    lane = lax.broadcasted_iota(jnp.int32, (toks, LANES), 1)
    block = jnp.where(lane < ny * nz, (lane % ny) * nz + lane // ny, -1).astype(F32)
    named = jnp.zeros((toks, LANES), F32)
    for k in range(ids.shape[1]):
        named = jnp.where(ids[:, k : k + 1] == block, 1.0, named)
    row = lax.broadcasted_iota(jnp.int32, (toks, toks), 0)
    col = lax.broadcasted_iota(jnp.int32, (toks, toks), 1)
    before = jnp.where(col < row, 1.0, 0.0).astype(BF16)
    position = jnp.dot(before, named.astype(BF16), preferred_element_type=F32)
    slots = jnp.where(named > 0.0, position, -1.0).astype(BF16)
    for k in range(ny):
        out_ref[k, :, 0:width] = tokens_ref[:, k * width : (k + 1) * width]
        out_ref[k, :, width : width + LANES] = slots
        out_ref[k, :, width + LANES : 2 * width + LANES] = w_out_ref[:, k * width : (k + 1) * width]
    base = 2 * width + LANES
    for k in range(ny):
        copies[k].wait()
        for g in range(part // toks):
            out_ref[k, :, base + g * LANES : base + (g + 1) * LANES] = in_rows[
                k, g * toks : (g + 1) * toks, :
            ]


def pack(where, tokens, ids, w_in, w_out, ny, nz, nt):
    toks, model = tokens.shape
    width = model // ny
    part = width // nt
    return pl.pallas_call(
        functools.partial(pack_kernel, ny=ny, nz=nz, nt=nt),
        out_shape=jax.ShapeDtypeStruct((ny, toks, 3 * width + LANES), BF16),
        grid_spec=pltpu.PrefetchScalarGridSpec(
            num_scalar_prefetch=1,
            grid=(1,),
            in_specs=[
                pl.BlockSpec((toks, model), lambda i, s: (0, 0)),
                pl.BlockSpec(ids.shape, lambda i, s: (0, 0)),
                pl.BlockSpec(memory_space=pl.ANY),
                pl.BlockSpec((w_out.shape[0] // nt, model), lambda i, s: (s[0], 0)),
            ],
            out_specs=pl.BlockSpec((ny, toks, 3 * width + LANES), lambda i, s: (0, 0, 0)),
            scratch_shapes=[
                pltpu.VMEM((ny, part, LANES), BF16),
                pltpu.SemaphoreType.DMA((ny,)),
            ],
        ),
        name="pack",
    )(where, tokens, ids, w_in, w_out)


def first_kernel(x_ref, pick_ref, w_ref, out_ref, wide, *, ny, nm, chunk, toks):
    nt, _, rows, lanes = w_ref.shape
    groups = lanes // LANES
    width = nt * rows * groups
    for t in range(nt):
        for g in range(groups):
            top = (t * groups + g) * rows
            for j in range(ny):
                wide[top : top + rows, j * LANES : (j + 1) * LANES] = w_ref[
                    t, j, :, g * LANES : (g + 1) * LANES
                ]
    per = chunk // toks * CAP
    band = ny * toks
    col = lax.broadcasted_iota(jnp.int32, (pick_ref.shape[0], chunk), 1)
    slot = lax.broadcasted_iota(jnp.int32, (per, chunk), 0).astype(F32)
    first = (col // toks * CAP).astype(F32)
    halves = x_ref.shape[0] // chunk // nm
    for m in range(x_ref.shape[0] // chunk):
        bands = [
            (m // halves) + nm * (m % halves * (chunk // band) + i) for i in range(chunk // band)
        ]
        x = jnp.concatenate([x_ref[r * band : (r + 1) * band, :] for r in bands], axis=0)
        h = jnp.dot(x[:, 0:width], wide[...], preferred_element_type=F32).astype(BF16)
        at = lax.dot_general(
            pick_ref[...],
            x[:, width : width + LANES],
            (((1,), (1,)), ((), ())),
            preferred_element_type=F32,
        )
        at = jnp.where(at >= 0.0, at + first, -1.0)
        for j in range(ny):
            s = jnp.where(slot == at[j : j + 1, :], 1.0, 0.0).astype(BF16)
            rows_j = jnp.dot(s, h[:, j * LANES : (j + 1) * LANES], preferred_element_type=F32)
            out_ref[j, m * per : (m + 1) * per, :] = rows_j.astype(BF16)


def first_product(x, pick, w, ny, nm, toks):
    chunk = 256
    slots = x.shape[0] // toks * CAP
    return pl.pallas_call(
        functools.partial(first_kernel, ny=ny, nm=nm, chunk=chunk, toks=toks),
        out_shape=jax.ShapeDtypeStruct((ny, slots, LANES), BF16),
        scratch_shapes=[pltpu.VMEM((x.shape[1] - LANES, ny * LANES), BF16)],
        name="first_product",
    )(x, pick, w)


def second_kernel(
    where_ref, h_ref, x_ref, pick_ref, w_ref, out_ref, tall, spread, *, ny, nm, chunk, toks
):
    zm = where_ref[1]
    nt, _, _, rows, width = w_ref.shape
    band = ny * toks
    blocks = nm * ny
    for q in range(nm):
        for j in range(ny):
            for t in range(nt):
                top = ((q * ny + j) * nt + t) * rows
                tall[top : top + rows, :] = w_ref[t, q, j]
    per = chunk // toks * CAP
    row = lax.broadcasted_iota(jnp.int32, (chunk, pick_ref.shape[0]), 0)
    slot = lax.broadcasted_iota(jnp.int32, (chunk, per), 1).astype(F32)
    first = (row // toks * CAP).astype(F32)
    for m in range(x_ref.shape[0] // chunk // nm):
        pos = []
        for i in range(chunk // band):
            top = (nm * (m * (chunk // band) + i) + zm) * band
            pos.append(x_ref[pl.ds(pl.multiple_of(top, band), band), :])
        at = lax.dot_general(
            jnp.concatenate(pos, axis=0),
            pick_ref[...],
            (((1,), (1,)), ((), ())),
            preferred_element_type=F32,
        )
        at = jnp.where(at >= 0.0, at + first, -1.0)
        for b in range(blocks):
            source = b % ny * nm + (zm + b // ny) % nm
            s = jnp.where(slot == at[:, b : b + 1], 1.0, 0.0).astype(BF16)
            full = jnp.dot(
                s, h_ref[source, m * per : (m + 1) * per, :], preferred_element_type=F32
            )
            spread[:, b * LANES : (b + 1) * LANES] = full.astype(BF16)
        out = jnp.dot(spread[...], tall[...], preferred_element_type=F32).astype(BF16)
        devices = chunk // toks
        out_ref[m * devices : (m + 1) * devices] = out.reshape(devices, toks, width)


def second_product(where, h, x, pick, w, ny, nm, toks):
    chunk = 256
    width = w.shape[-1]
    total = x.shape[0]
    devices = total // toks // nm
    return pl.pallas_call(
        functools.partial(second_kernel, ny=ny, nm=nm, chunk=chunk, toks=toks),
        out_shape=jax.ShapeDtypeStruct((devices, toks, width), BF16),
        grid_spec=pltpu.PrefetchScalarGridSpec(
            num_scalar_prefetch=1,
            grid=(1,),
            in_specs=[
                pl.BlockSpec(h.shape, lambda i, s: (0, 0, 0)),
                pl.BlockSpec((total, LANES), lambda i, s: (0, width // LANES)),
                pl.BlockSpec(pick.shape, lambda i, s: (0, 0)),
                pl.BlockSpec(w.shape, lambda i, s: (0,) * 5),
            ],
            out_specs=pl.BlockSpec((devices, toks, width), lambda i, s: (0, 0, 0)),
            scratch_shapes=[
                pltpu.VMEM((nm * ny * LANES, width), BF16),
                pltpu.VMEM((chunk, nm * ny * LANES), BF16),
            ],
        ),
        name="second_product",
    )(where, h, x, pick, w)


def combine_kernel(y_ref, out_ref, *, ny):
    width = y_ref.shape[2]
    for k in range(ny):
        total = y_ref[k].astype(F32)
        for other in range(ny + k, y_ref.shape[0], ny):
            total = total + y_ref[other].astype(F32)
        out_ref[:, k * width : (k + 1) * width] = total.astype(BF16)


def combine(y, ny):
    return pl.pallas_call(
        functools.partial(combine_kernel, ny=ny),
        out_shape=jax.ShapeDtypeStruct((y.shape[1], y.shape[2] * ny), BF16),
        name="combine",
    )(y)


def near(value):
    return pltpu.with_memory_space_constraint(value, pltpu.VMEM)


def body(tokens, block_ids, w_in, bias_in, w_out):
    toks = tokens.shape[0]
    plane = ("zn", "zm")
    ny, nm = lax.axis_size("y"), lax.axis_size("zm")
    nz = lax.axis_size("zn") * nm
    nt = lax.axis_size("x") * lax.axis_size("c")
    width = tokens.shape[1] // ny
    share = lax.axis_index("x") * lax.axis_size("c") + lax.axis_index("c")
    zn, zm = lax.axis_index("zn"), lax.axis_index("zm")
    where = jnp.stack([share, zm]).astype(jnp.int32)

    payload = pack(where, tokens, block_ids.T, w_in, w_out, ny, nz, nt)
    got = lax.all_to_all(payload, "y", split_axis=0, concat_axis=0, tiled=True)
    x_part = got[:, :, : width + LANES].reshape(ny * toks, width + LANES)
    x = lax.all_gather(x_part, plane, axis=0, tiled=True)
    w1 = got[:, :, 2 * width + LANES :]
    w1 = lax.all_to_all(
        jnp.broadcast_to(w1[None], (nt,) + w1.shape), ("x", "c"), split_axis=0, concat_axis=0, tiled=True
    )
    w2 = got[:, :, width + LANES : 2 * width + LANES]
    w2 = jnp.stack([w2] + [lax.ppermute(w2, "zm", [(i, (i - k) % nm) for i in range(nm)]) for k in range(1, nm)])
    x, w1, w2 = lax.optimization_barrier((x, w1, w2))
    w2 = lax.all_gather(w2[None], ("x", "c"), axis=0, tiled=True)

    lane = jnp.arange(LANES, dtype=jnp.int32)[None, :]
    block = jnp.arange(nm * ny, dtype=jnp.int32)[:, None]
    group = zn * nm + (zm + block // ny) % nm
    pick2 = (lane == group * ny + block % ny).astype(BF16)
    pick1 = ((lane == (zn * nm + zm) * ny + block) & (block < ny)).astype(BF16)

    h = first_product(x, pick1, near(w1), ny, nm, toks)
    h = lax.all_to_all(h, "y", split_axis=0, concat_axis=0, tiled=True)
    h = jnp.sum(h.astype(F32), axis=0) + bias_in[None, :]
    h = jnp.maximum(h, 0.0).astype(BF16)
    h = h.reshape(1, nm, h.shape[0] // nm, LANES)
    h = jnp.broadcast_to(h, (ny,) + h.shape[1:]).reshape((ny * nm,) + h.shape[2:])
    h = lax.all_to_all(h, ("y", "zm"), split_axis=0, concat_axis=0, tiled=True)
    y = second_product(where, near(h), x, pick2, w2, ny, nm, toks)
    y = lax.all_to_all(y, ("zn", "y"), split_axis=0, concat_axis=0, tiled=True)
    return combine(near(y), ny)


def solution(mesh):
    side = math.isqrt(mesh.shape["blk"])
    cores, pair = 2, 2
    fine = Mesh(
        mesh.devices.reshape(side, side // pair, pair, mesh.shape["tok"] // cores, cores),
        ("y", "zn", "zm", "x", "c"),
    )
    rows = ("x", "c", "y", "zn", "zm")
    blocks = ("y", "zn", "zm")
    return jax.shard_map(
        body,
        mesh=fine,
        in_specs=(P(rows, None), P(rows, None), P(None, blocks), P(blocks), P(blocks, None)),
        out_specs=P(rows, None),
        check_vma=False,
    )
```

```python
import functools
import math

import jax
import jax.numpy as jnp
from jax import lax
from jax.experimental import pallas as pl
from jax.experimental.pallas import tpu as pltpu
from jax.sharding import Mesh
from jax.sharding import PartitionSpec as P

CAP = 5
LANES = 128
CHUNK = 256
BF16 = jnp.bfloat16
F32 = jnp.float32
ANY = pl.BlockSpec(memory_space=pl.ANY)
VMEM = pl.BlockSpec(memory_space=pltpu.VMEM)


def sizes():
    ny, nn, nm = lax.axis_size("y"), lax.axis_size("zn"), lax.axis_size("zm")
    return ny, nn, nm, lax.axis_size("x"), lax.axis_size("c")


def near(value):
    return pltpu.with_memory_space_constraint(value, pltpu.VMEM)


def pack_kernel(tokens_ref, ids_ref, w_in_ref, w_out_ref, out_ref, w2_ref, in_rows, sems, *, dims):
    ny, nn, nm, nx, nc = dims
    nz, nt = nn * nm, nx * nc
    share = lax.axis_index("x") * nc + lax.axis_index("c")
    width = tokens_ref.shape[1] // ny
    part = width // nt
    toks = tokens_ref.shape[0]
    rows = w_out_ref.shape[0] // nt
    copies = []
    for k in range(ny):
        top = pl.multiple_of(k * width + share * part, 16)
        copies.append(
            pltpu.make_async_copy(w_in_ref.at[pl.ds(top, part), :], in_rows.at[k], sems.at[0, k])
        )
    for k in range(ny):
        cut = pl.ds(k * width, width)
        copies.append(
            pltpu.make_async_copy(
                tokens_ref.at[:, cut], out_ref.at[k, :, pl.ds(0, width)], sems.at[1, k]
            )
        )
        for m in range(nm):
            top = pl.multiple_of(share * rows, 16)
            copies.append(
                pltpu.make_async_copy(
                    w_out_ref.at[pl.ds(top, rows), cut], w2_ref.at[k * nm + m], sems.at[2 + m, k]
                )
            )
    for c in copies:
        c.start()
    same = lax.broadcasted_iota(jnp.int32, (ids_ref.shape[0],) * 2, 0)
    same = same == lax.broadcasted_iota(jnp.int32, same.shape, 1)
    ids = lax.dot_general(
        ids_ref[...].astype(F32).astype(BF16),
        jnp.where(same, 1.0, 0.0).astype(BF16),
        (((0,), (0,)), ((), ())),
        preferred_element_type=F32,
    )
    lane = lax.broadcasted_iota(jnp.int32, (toks, LANES), 1)
    block = jnp.where(lane < ny * nz, (lane % ny) * nz + lane // ny, -1).astype(F32)
    named = jnp.zeros((toks, LANES), F32)
    for k in range(ids.shape[1]):
        named = jnp.where(ids[:, k : k + 1] == block, 1.0, named)
    row = lax.broadcasted_iota(jnp.int32, (toks, toks), 0)
    col = lax.broadcasted_iota(jnp.int32, (toks, toks), 1)
    before = jnp.where(col < row, 1.0, 0.0).astype(BF16)
    position = jnp.dot(before, named.astype(BF16), preferred_element_type=F32)
    slots = jnp.where(named > 0.0, position, -1.0).astype(BF16)
    base = width + LANES
    for k in range(ny):
        out_ref[k, :, width:base] = slots
    for k in range(ny):
        copies[k].wait()
        for g in range(part // toks):
            out_ref[k, :, base + g * LANES : base + (g + 1) * LANES] = in_rows[
                k, g * toks : (g + 1) * toks, :
            ]
    for c in copies[ny:]:
        c.wait()


def pack(tokens, ids, w_in, w_out, dims):
    ny, _, nm, nx, nc = dims
    toks, model = tokens.shape
    width = model // ny
    rows = w_out.shape[0] // (nx * nc)
    return pl.pallas_call(
        functools.partial(pack_kernel, dims=dims),
        out_shape=(
            jax.ShapeDtypeStruct((ny, toks, 2 * width + LANES), BF16),
            jax.ShapeDtypeStruct((ny * nm, rows, width), BF16),
        ),
        in_specs=[ANY, VMEM, ANY, ANY],
        out_specs=(VMEM, VMEM),
        scratch_shapes=[
            pltpu.VMEM((ny, width // (nx * nc), LANES), BF16),
            pltpu.SemaphoreType.DMA((2 + nm, ny)),
        ],
        name="pack",
    )(tokens, ids, w_in, w_out)


def tile_kernel(mine_ref, other_ref, wide_ref, *, dims):
    ny, _, _, nx, nc = dims
    x, c = lax.axis_index("x"), lax.axis_index("c")
    rows, width = mine_ref.shape[2:]
    groups = width // LANES
    for source, core in ((mine_ref, c), (other_ref, nc - 1 - c)):
        for s in range(nx):
            share = (x + nx - s) % nx * nc + core
            for g in range(groups):
                top = pl.multiple_of((share * groups + g) * rows, 16)
                for k in range(ny):
                    wide_ref[pl.ds(top, rows), k * LANES : (k + 1) * LANES] = source[
                        s, k, :, g * LANES : (g + 1) * LANES
                    ]


def tile(mine, other, dims):
    ny, width = dims[0], mine.shape[3]
    return pl.pallas_call(
        functools.partial(tile_kernel, dims=dims),
        out_shape=jax.ShapeDtypeStruct((width, ny * LANES), BF16),
        in_specs=[VMEM, VMEM],
        out_specs=VMEM,
        name="tile",
    )(mine, other)


def first_kernel(x_ref, wide_ref, out_ref, wide, bands, wide_sem, sems, *, dims, toks):
    ny, nn, nm, _, _ = dims
    width = wide_ref.shape[0]
    weight = pltpu.make_async_copy(wide_ref, wide, wide_sem)
    weight.start()
    band = ny * toks
    order = [a * nm + m for m in range(nm) for a in range(nn)]
    copies = {
        r: pltpu.make_async_copy(x_ref.at[pl.ds(r * band, band), :], bands.at[r], sems.at[r])
        for r in order
    }
    for r in order:
        copies[r].start()
    per = CHUNK // toks * CAP
    base = (lax.axis_index("zn") * nm + lax.axis_index("zm")) * ny
    row = lax.broadcasted_iota(jnp.int32, (16, LANES), 0)
    lane = lax.broadcasted_iota(jnp.int32, (16, LANES), 1)
    pick = jnp.where((lane == base + row) & (row < ny), 1.0, 0.0).astype(BF16)
    col = lax.broadcasted_iota(jnp.int32, (16, CHUNK), 1)
    slot = lax.broadcasted_iota(jnp.int32, (per, CHUNK), 0).astype(F32)
    first = (col // toks * CAP).astype(F32)
    step = CHUNK // band
    weight.wait()
    for m in range(len(order) // step):
        used = order[m * step : (m + 1) * step]
        for r in used:
            copies[r].wait()
        x = jnp.concatenate([bands[r] for r in used], axis=0)
        h = jnp.dot(x[:, 0:width], wide[...], preferred_element_type=F32).astype(BF16)
        at = lax.dot_general(
            pick, x[:, width : width + LANES], (((1,), (1,)), ((), ())), preferred_element_type=F32
        )
        at = jnp.where(at >= 0.0, at + first, -1.0)
        for j in range(ny):
            s = jnp.where(slot == at[j : j + 1, :], 1.0, 0.0).astype(BF16)
            rows_j = jnp.dot(s, h[:, j * LANES : (j + 1) * LANES], preferred_element_type=F32)
            out_ref[j, m * per : (m + 1) * per, :] = rows_j.astype(BF16)


def first_product(x, wide, dims, toks):
    ny, nn, nm, _, _ = dims
    slots = x.shape[0] // toks * CAP
    return pl.pallas_call(
        functools.partial(first_kernel, dims=dims, toks=toks),
        out_shape=jax.ShapeDtypeStruct((ny, slots, LANES), BF16),
        in_specs=[ANY, ANY],
        out_specs=VMEM,
        scratch_shapes=[
            pltpu.VMEM(wide.shape, BF16),
            pltpu.VMEM((nn * nm, ny * toks, x.shape[1]), BF16),
            pltpu.SemaphoreType.DMA,
            pltpu.SemaphoreType.DMA((nn * nm,)),
        ],
        name="first_product",
    )(x, wide)


def activate_kernel(part_ref, bias_ref, out_ref, *, dims):
    ny, _, nm, _, _ = dims
    rows = out_ref.shape[1]
    for m in range(nm):
        total = part_ref[0, m * rows : (m + 1) * rows, :].astype(F32)
        for k in range(1, ny):
            total = total + part_ref[k, m * rows : (m + 1) * rows, :].astype(F32)
        h = jnp.maximum(total + bias_ref[...], 0.0).astype(BF16)
        for k in range(ny):
            out_ref[k * nm + m] = h


def activate(part, bias, dims):
    ny, _, nm, _, _ = dims
    return pl.pallas_call(
        functools.partial(activate_kernel, dims=dims),
        out_shape=jax.ShapeDtypeStruct((ny * nm, part.shape[1] // nm, LANES), BF16),
        in_specs=[VMEM, VMEM],
        out_specs=VMEM,
        name="activate",
    )(part, bias)


def second_kernel(h_ref, x_ref, w_ref, out_ref, tall, spread, places, sems, place_sems, *, dims, toks):
    ny, nn, nm, _, _ = dims
    zn, zm = lax.axis_index("zn"), lax.axis_index("zm")
    blocks, nt, rows, width = tall.shape
    band = ny * toks
    marks = []
    for a in range(nn):
        top = pl.multiple_of((a * nm + zm) * band, band)
        marks.append(
            pltpu.make_async_copy(
                x_ref.at[pl.ds(top, band), pl.ds(width, LANES)], places.at[a], place_sems.at[a]
            )
        )
    copies = [
        pltpu.make_async_copy(w_ref.at[:, b], tall.at[b], sems.at[b]) for b in range(blocks)
    ]
    for c in marks + copies:
        c.start()
    per = CHUNK // toks * CAP
    row = lax.broadcasted_iota(jnp.int32, (16, LANES), 0)
    lane = lax.broadcasted_iota(jnp.int32, (16, LANES), 1)
    pick = lane == (zn * nm + row % nm) * ny + row // nm
    pick = jnp.where(pick & (row < blocks), 1.0, 0.0).astype(BF16)
    row = lax.broadcasted_iota(jnp.int32, (CHUNK, 16), 0)
    slot = lax.broadcasted_iota(jnp.int32, (CHUNK, per), 1).astype(F32)
    first = (row // toks * CAP).astype(F32)
    step = CHUNK // band
    for c in marks:
        c.wait()
    for m in range(nn // step):
        at = lax.dot_general(
            jnp.concatenate([places[m * step + i] for i in range(step)], axis=0),
            pick,
            (((1,), (1,)), ((), ())),
            preferred_element_type=F32,
        )
        at = jnp.where(at >= 0.0, at + first, -1.0)
        for b in range(blocks):
            s = jnp.where(slot == at[:, b : b + 1], 1.0, 0.0).astype(BF16)
            full = jnp.dot(s, h_ref[b, m * per : (m + 1) * per, :], preferred_element_type=F32)
            spread[m * CHUNK : (m + 1) * CHUNK, b * LANES : (b + 1) * LANES] = full.astype(BF16)
    for c in copies:
        c.wait()
    devices = CHUNK // toks
    for m in range(nn // step):
        out = jnp.dot(
            spread[m * CHUNK : (m + 1) * CHUNK, :],
            tall[...].reshape(blocks * nt * rows, width),
            preferred_element_type=F32,
        )
        out_ref[m * devices : (m + 1) * devices] = out.astype(BF16).reshape(devices, toks, width)


def second_product(h, x, w, dims, toks):
    ny, nn, nm, nx, nc = dims
    rows, width = w.shape[2:]
    return pl.pallas_call(
        functools.partial(second_kernel, dims=dims, toks=toks),
        out_shape=jax.ShapeDtypeStruct((ny * nn, toks, width), BF16),
        in_specs=[VMEM, ANY, ANY],
        out_specs=VMEM,
        scratch_shapes=[
            pltpu.VMEM((ny * nm, nx * nc, rows, width), BF16),
            pltpu.VMEM((ny * nn * toks, ny * nm * LANES), BF16),
            pltpu.VMEM((nn, ny * toks, LANES), BF16),
            pltpu.SemaphoreType.DMA((ny * nm,)),
            pltpu.SemaphoreType.DMA((nn,)),
        ],
        name="second_product",
    )(h, x, w)


def combine_kernel(y_ref, out_ref, *, ny):
    width = y_ref.shape[2]
    for k in range(ny):
        total = y_ref[k].astype(F32)
        for other in range(ny + k, y_ref.shape[0], ny):
            total = total + y_ref[other].astype(F32)
        out_ref[:, k * width : (k + 1) * width] = total.astype(BF16)


def combine(y, ny):
    return pl.pallas_call(
        functools.partial(combine_kernel, ny=ny),
        out_shape=jax.ShapeDtypeStruct((y.shape[1], y.shape[2] * ny), BF16),
        in_specs=[VMEM],
        out_specs=VMEM,
        name="combine",
    )(y)


def exchange(value, axes):
    return lax.all_to_all(value, axes, split_axis=0, concat_axis=0, tiled=True)


def body(tokens, block_ids, w_in, bias_in, w_out):
    dims = sizes()
    ny, _, _, nx, nc = dims
    toks = tokens.shape[0]
    width = tokens.shape[1] // ny

    payload, w2 = pack(tokens, block_ids.T, w_in, w_out, dims)
    got = exchange(payload, "y")
    x = lax.all_gather(
        got[:, :, : width + LANES].reshape(ny * toks, width + LANES), ("zn", "zm"), axis=0, tiled=True
    )
    w1 = got[:, :, width + LANES :]
    w2, w1 = lax.optimization_barrier((w2, w1))
    w2 = exchange(w2, ("y", "zm"))
    mine = [w1]
    for s in range(1, nx):
        mine.append(lax.ppermute(w1, "x", [(i, (i + s) % nx) for i in range(nx)]))
    mine = jnp.stack(mine)
    other = lax.ppermute(mine, "c", [(i, nc - 1 - i) for i in range(nc)])
    wide = tile(near(mine), near(other), dims)
    x, wide, w2 = lax.optimization_barrier((x, wide, w2))
    w2 = lax.all_gather(w2[None], ("x", "c"), axis=0, tiled=True)

    h = exchange(first_product(x, wide, dims, toks), "y")
    h = exchange(activate(near(h), bias_in[None, :], dims), ("y", "zm"))
    y = exchange(second_product(near(h), x, w2, dims, toks), ("zn", "y"))
    return combine(near(y), ny)


def solution(mesh):
    side = math.isqrt(mesh.shape["blk"])
    cores, pair = 2, 2
    fine = Mesh(
        mesh.devices.reshape(side, side // pair, pair, mesh.shape["tok"] // cores, cores),
        ("y", "zn", "zm", "x", "c"),
    )
    rows = ("x", "c", "y", "zn", "zm")
    blocks = ("y", "zn", "zm")
    return jax.shard_map(
        body,
        mesh=fine,
        in_specs=(P(rows, None), P(rows, None), P(None, blocks), P(blocks), P(blocks, None)),
        out_specs=P(rows, None),
        check_vma=False,
    )
```

```python
import functools
import math

import jax
import jax.numpy as jnp
from jax import lax
from jax.experimental import pallas as pl
from jax.experimental.pallas import tpu as pltpu
from jax.sharding import Mesh
from jax.sharding import PartitionSpec as P


CAP = 5
LANES = 128
CHUNK = 256
BF16 = jnp.bfloat16
F32 = jnp.float32
HBM = pl.BlockSpec(memory_space=pltpu.HBM)
VMEM = pl.BlockSpec(memory_space=pltpu.VMEM)


def sizes():
    ny, nn, nm = lax.axis_size("y"), lax.axis_size("zn"), lax.axis_size("zm")
    return ny, nn, nm, lax.axis_size("x"), lax.axis_size("c")


def room(mebibytes):
    return pltpu.CompilerParams(vmem_limit_bytes=mebibytes << 20)


def near(value):
    return pltpu.with_memory_space_constraint(value, pltpu.VMEM)


def pack_kernel(tokens_ref, ids_ref, w_in_ref, w_out_ref, out_ref, w2_ref, in_rows, sems, *, dims):
    ny, nn, nm, nx, nc = dims
    nz, nt = nn * nm, nx * nc
    share = lax.axis_index("x") * nc + lax.axis_index("c")
    width = tokens_ref.shape[1] // ny
    part = width // nt
    toks = tokens_ref.shape[0]
    rows = w_out_ref.shape[0] // nt
    copies = []
    for k in range(ny):
        top = pl.multiple_of(k * width + share * part, 16)
        copies.append(
            pltpu.make_async_copy(w_in_ref.at[pl.ds(top, part), :], in_rows.at[k], sems.at[0, k])
        )
    for k in range(ny):
        cut = pl.ds(k * width, width)
        copies.append(
            pltpu.make_async_copy(
                tokens_ref.at[:, cut], out_ref.at[k, :, pl.ds(0, width)], sems.at[1, k]
            )
        )
        for m in range(nm):
            top = pl.multiple_of(share * rows, 16)
            copies.append(
                pltpu.make_async_copy(
                    w_out_ref.at[pl.ds(top, rows), cut], w2_ref.at[k * nm + m], sems.at[2 + m, k]
                )
            )
    for c in copies:
        c.start()
    same = lax.broadcasted_iota(jnp.int32, (ids_ref.shape[0],) * 2, 0)
    same = same == lax.broadcasted_iota(jnp.int32, same.shape, 1)
    ids = lax.dot_general(
        ids_ref[...].astype(F32).astype(BF16),
        jnp.where(same, 1.0, 0.0).astype(BF16),
        (((0,), (0,)), ((), ())),
        preferred_element_type=F32,
    )
    lane = lax.broadcasted_iota(jnp.int32, (toks, LANES), 1)
    block = jnp.where(lane < ny * nz, (lane % ny) * nz + lane // ny, -1).astype(F32)
    named = jnp.zeros((toks, LANES), F32)
    for k in range(ids.shape[1]):
        named = jnp.where(ids[:, k : k + 1] == block, 1.0, named)
    row = lax.broadcasted_iota(jnp.int32, (toks, toks), 0)
    col = lax.broadcasted_iota(jnp.int32, (toks, toks), 1)
    before = jnp.where(col < row, 1.0, 0.0).astype(BF16)
    position = jnp.dot(before, named.astype(BF16), preferred_element_type=F32)
    slots = jnp.where(named > 0.0, position, -1.0).astype(BF16)
    base = width + LANES
    for k in range(ny):
        out_ref[k, :, width:base] = slots
    for k in range(ny):
        copies[k].wait()
        for g in range(part // toks):
            out_ref[k, :, base + g * LANES : base + (g + 1) * LANES] = in_rows[
                k, g * toks : (g + 1) * toks, :
            ]
    for c in copies[ny:]:
        c.wait()


def pack(tokens, ids, w_in, w_out, dims):
    ny, _, nm, nx, nc = dims
    toks, model = tokens.shape
    width = model // ny
    rows = w_out.shape[0] // (nx * nc)
    return pl.pallas_call(
        functools.partial(pack_kernel, dims=dims),
        out_shape=(
            pltpu.VMEM((ny, toks, 2 * width + LANES), BF16),
            jax.ShapeDtypeStruct((ny * nm, rows, width), BF16),
        ),
        in_specs=[HBM, VMEM, HBM, HBM],
        out_specs=(VMEM, VMEM),
        scratch_shapes=[
            pltpu.VMEM((ny, width // (nx * nc), LANES), BF16),
            pltpu.SemaphoreType.DMA((2 + nm, ny)),
        ],
        name="pack",
    )(tokens, ids, w_in, w_out)


def tile_kernel(mine_ref, other_ref, wide_ref, *, dims):
    ny, _, _, nx, nc = dims
    x, c = lax.axis_index("x"), lax.axis_index("c")
    rows, width = mine_ref.shape[2:]
    groups = width // LANES
    for source, core in ((mine_ref, c), (other_ref, nc - 1 - c)):
        for s in range(nx):
            share = (x + nx - s) % nx * nc + core
            for g in range(groups):
                top = pl.multiple_of((share * groups + g) * rows, 16)
                for k in range(ny):
                    wide_ref[pl.ds(top, rows), k * LANES : (k + 1) * LANES] = source[
                        s, k, :, g * LANES : (g + 1) * LANES
                    ]


def tile(mine, other, dims):
    ny, width = dims[0], mine.shape[3]
    return pl.pallas_call(
        functools.partial(tile_kernel, dims=dims),
        out_shape=pltpu.VMEM((width, ny * LANES), BF16),
        in_specs=[VMEM, VMEM],
        out_specs=VMEM,
        compiler_params=room(56),
        name="tile",
    )(mine, other)


def first_kernel(x_ref, wide_ref, out_ref, bands, sems, *, dims, toks):
    ny, nn, nm, _, _ = dims
    width = wide_ref.shape[0]
    band = ny * toks
    order = [a * nm + m for m in range(nm) for a in range(nn)]
    copies = {
        r: pltpu.make_async_copy(x_ref.at[pl.ds(r * band, band), :], bands.at[r], sems.at[r])
        for r in order
    }
    for r in order:
        copies[r].start()
    per = CHUNK // toks * CAP
    base = (lax.axis_index("zn") * nm + lax.axis_index("zm")) * ny
    row = lax.broadcasted_iota(jnp.int32, (16, LANES), 0)
    lane = lax.broadcasted_iota(jnp.int32, (16, LANES), 1)
    pick = jnp.where((lane == base + row) & (row < ny), 1.0, 0.0).astype(BF16)
    col = lax.broadcasted_iota(jnp.int32, (16, CHUNK), 1)
    slot = lax.broadcasted_iota(jnp.int32, (per, CHUNK), 0).astype(F32)
    first = (col // toks * CAP).astype(F32)
    step = CHUNK // band
    for m in range(len(order) // step):
        used = order[m * step : (m + 1) * step]
        for r in used:
            copies[r].wait()
        x = jnp.concatenate([bands[r] for r in used], axis=0)
        h = jnp.dot(x[:, 0:width], wide_ref[...], preferred_element_type=F32).astype(BF16)
        at = lax.dot_general(
            pick, x[:, width : width + LANES], (((1,), (1,)), ((), ())), preferred_element_type=F32
        )
        at = jnp.where(at >= 0.0, at + first, -1.0)
        for j in range(ny):
            s = jnp.where(slot == at[j : j + 1, :], 1.0, 0.0).astype(BF16)
            rows_j = jnp.dot(s, h[:, j * LANES : (j + 1) * LANES], preferred_element_type=F32)
            out_ref[j, m * per : (m + 1) * per, :] = rows_j.astype(BF16)


def first_product(x, wide, dims, toks):
    ny, nn, nm, _, _ = dims
    slots = x.shape[0] // toks * CAP
    return pl.pallas_call(
        functools.partial(first_kernel, dims=dims, toks=toks),
        out_shape=pltpu.VMEM((ny, slots, LANES), BF16),
        in_specs=[HBM, VMEM],
        out_specs=VMEM,
        scratch_shapes=[
            pltpu.VMEM((nn * nm, ny * toks, x.shape[1]), BF16),
            pltpu.SemaphoreType.DMA((nn * nm,)),
        ],
        name="first_product",
    )(x, wide)


def activate_kernel(part_ref, bias_ref, out_ref, *, dims):
    ny, _, nm, _, _ = dims
    rows = out_ref.shape[1]
    for m in range(nm):
        total = part_ref[0, m * rows : (m + 1) * rows, :].astype(F32)
        for k in range(1, ny):
            total = total + part_ref[k, m * rows : (m + 1) * rows, :].astype(F32)
        h = jnp.maximum(total + bias_ref[...], 0.0).astype(BF16)
        for k in range(ny):
            out_ref[k * nm + m] = h


def activate(part, bias, dims):
    ny, _, nm, _, _ = dims
    return pl.pallas_call(
        functools.partial(activate_kernel, dims=dims),
        out_shape=pltpu.VMEM((ny * nm, part.shape[1] // nm, LANES), BF16),
        in_specs=[VMEM, VMEM],
        out_specs=VMEM,
        name="activate",
    )(part, bias)


def place_kernel(x_ref, place_ref, marks, sems, *, dims, toks):
    ny, nn, nm, _, _ = dims
    zn, zm = lax.axis_index("zn"), lax.axis_index("zm")
    width = x_ref.shape[1] - LANES
    blocks = ny * nm
    band = ny * toks
    copies = []
    for a in range(nn):
        top = pl.multiple_of((a * nm + zm) * band, band)
        copies.append(
            pltpu.make_async_copy(
                x_ref.at[pl.ds(top, band), pl.ds(width, LANES)], marks.at[a], sems.at[a]
            )
        )
    for c in copies:
        c.start()
    per = CHUNK // toks * CAP
    row = lax.broadcasted_iota(jnp.int32, (blocks, LANES), 0)
    lane = lax.broadcasted_iota(jnp.int32, (blocks, LANES), 1)
    pick = jnp.where(lane == (zn * nm + row % nm) * ny + row // nm, 1.0, 0.0).astype(BF16)
    row = lax.broadcasted_iota(jnp.int32, (CHUNK, blocks), 0)
    slot = lax.broadcasted_iota(jnp.int32, (CHUNK, per), 1).astype(F32)
    first = (row // toks * CAP).astype(F32)
    step = CHUNK // band
    for c in copies:
        c.wait()
    for m in range(nn // step):
        at = lax.dot_general(
            jnp.concatenate([marks[m * step + i] for i in range(step)], axis=0),
            pick,
            (((1,), (1,)), ((), ())),
            preferred_element_type=F32,
        )
        at = jnp.where(at >= 0.0, at + first, -1.0)
        for b in range(blocks):
            place_ref[m, b] = jnp.where(slot == at[:, b : b + 1], 1.0, 0.0).astype(BF16)


def place(x, dims, toks):
    ny, nn, nm, _, _ = dims
    band = ny * toks
    return pl.pallas_call(
        functools.partial(place_kernel, dims=dims, toks=toks),
        out_shape=pltpu.VMEM((nn * band // CHUNK, ny * nm, CHUNK, CHUNK // toks * CAP), BF16),
        in_specs=[HBM],
        out_specs=VMEM,
        scratch_shapes=[
            pltpu.VMEM((nn, band, LANES), BF16),
            pltpu.SemaphoreType.DMA((nn,)),
        ],
        name="place",
    )(x)


def second_kernel(h_ref, place_ref, w_ref, out_ref, tall, spread, sems, *, toks):
    chunks, blocks, _, per = place_ref.shape
    width = w_ref.shape[3]
    devices = CHUNK // toks
    copies = [
        pltpu.make_async_copy(w_ref.at[:, b], tall.at[b], sems.at[b]) for b in range(blocks)
    ]
    for c in copies:
        c.start()
    for m in range(chunks):
        for b in range(blocks):
            full = jnp.dot(
                place_ref[m, b], h_ref[b, m * per : (m + 1) * per, :], preferred_element_type=F32
            )
            spread[m, :, b * LANES : (b + 1) * LANES] = full.astype(BF16)
    for c in copies:
        c.wait()
    for m in range(chunks):
        out = jnp.dot(
            spread[m], tall[...].reshape(blocks * LANES, width), preferred_element_type=F32
        )
        out_ref[m * devices : (m + 1) * devices] = out.astype(BF16).reshape(devices, toks, width)


def second_product(h, places, w, toks):
    chunks, blocks = places.shape[:2]
    nt, _, rows, width = w.shape
    return pl.pallas_call(
        functools.partial(second_kernel, toks=toks),
        out_shape=pltpu.VMEM((chunks * CHUNK // toks, toks, width), BF16),
        in_specs=[VMEM, VMEM, HBM],
        out_specs=VMEM,
        scratch_shapes=[
            pltpu.VMEM((blocks, nt, rows, width), BF16),
            pltpu.VMEM((chunks, CHUNK, blocks * LANES), BF16),
            pltpu.SemaphoreType.DMA((blocks,)),
        ],
        compiler_params=room(58),
        name="second_product",
    )(h, places, w)


def combine_kernel(y_ref, out_ref, *, ny):
    width = y_ref.shape[2]
    for k in range(ny):
        total = y_ref[k].astype(F32)
        for other in range(ny + k, y_ref.shape[0], ny):
            total = total + y_ref[other].astype(F32)
        out_ref[:, k * width : (k + 1) * width] = total.astype(BF16)


def combine(y, ny):
    return pl.pallas_call(
        functools.partial(combine_kernel, ny=ny),
        out_shape=jax.ShapeDtypeStruct((y.shape[1], y.shape[2] * ny), BF16),
        in_specs=[VMEM],
        out_specs=VMEM,
        name="combine",
    )(y)


def exchange(value, axes):
    return lax.all_to_all(value, axes, split_axis=0, concat_axis=0, tiled=True)


def body(tokens, block_ids, w_in, bias_in, w_out):
    dims = sizes()
    ny, _, _, nx, nc = dims
    toks = tokens.shape[0]
    width = tokens.shape[1] // ny

    payload, w2 = pack(tokens, block_ids.T, w_in, w_out, dims)
    got = exchange(payload, "y")
    x = lax.all_gather(
        got[:, :, : width + LANES].reshape(ny * toks, width + LANES), ("zn", "zm"), axis=0, tiled=True
    )
    w1 = got[:, :, width + LANES :]
    w2, w1 = lax.optimization_barrier((w2, w1))
    w2 = exchange(w2, ("y", "zm"))
    mine = [w1]
    for s in range(1, nx):
        mine.append(lax.ppermute(w1, "x", [(i, (i + s) % nx) for i in range(nx)]))
    mine = jnp.stack(mine)
    other = lax.ppermute(mine, "c", [(i, nc - 1 - i) for i in range(nc)])
    wide = tile(near(mine), near(other), dims)
    x, wide, w2 = lax.optimization_barrier((x, wide, w2))
    w2 = lax.all_gather(w2[None], ("x", "c"), axis=0, tiled=True)

    h = exchange(first_product(x, near(wide), dims, toks), "y")
    h = activate(near(h), bias_in[None, :], dims)
    h = exchange(h, ("y", "zm"))
    places = place(x, dims, toks)
    y = exchange(second_product(near(h), near(places), w2, toks), ("zn", "y"))
    return combine(near(y), ny)


def solution(mesh):
    side = math.isqrt(mesh.shape["blk"])
    cores, pair = 2, 2
    fine = Mesh(
        mesh.devices.reshape(side, side // pair, pair, mesh.shape["tok"] // cores, cores),
        ("y", "zn", "zm", "x", "c"),
    )
    rows = ("x", "c", "y", "zn", "zm")
    blocks = ("y", "zn", "zm")
    return jax.shard_map(
        body,
        mesh=fine,
        in_specs=(P(rows, None), P(rows, None), P(None, blocks), P(blocks), P(blocks, None)),
        out_specs=P(rows, None),
        check_vma=False,
    )
```

```python
import functools
import math

import jax
import jax.numpy as jnp
from jax import lax
from jax.experimental import pallas as pl
from jax.experimental.pallas import tpu as pltpu
from jax.sharding import Mesh
from jax.sharding import PartitionSpec as P


CAP = 5
LANES = 128
CHUNK = 256
BF16 = jnp.bfloat16
F32 = jnp.float32
HBM = pl.BlockSpec(memory_space=pltpu.HBM)
VMEM = pl.BlockSpec(memory_space=pltpu.VMEM)


def sizes():
    ny, nn, nm = lax.axis_size("y"), lax.axis_size("zn"), lax.axis_size("zm")
    return ny, nn, nm, lax.axis_size("x"), lax.axis_size("c")


def room(mebibytes):
    return pltpu.CompilerParams(vmem_limit_bytes=mebibytes << 20)


def near(value):
    return pltpu.with_memory_space_constraint(value, pltpu.VMEM)


def pack_kernel(tokens_ref, ids_ref, w_in_ref, out_ref, in_rows, sems, *, dims):
    ny, nn, nm, nx, nc = dims
    nz, nt = nn * nm, nx * nc
    share = lax.axis_index("x") * nc + lax.axis_index("c")
    width = tokens_ref.shape[1] // ny
    part = width // nt
    toks = tokens_ref.shape[0]
    copies = []
    for k in range(ny):
        top = pl.multiple_of(k * width + share * part, 16)
        copies.append(
            pltpu.make_async_copy(w_in_ref.at[pl.ds(top, part), :], in_rows.at[k], sems.at[0, k])
        )
    for k in range(ny):
        cut = pl.ds(k * width, width)
        copies.append(
            pltpu.make_async_copy(
                tokens_ref.at[:, cut], out_ref.at[k, :, pl.ds(0, width)], sems.at[1, k]
            )
        )
    for c in copies:
        c.start()
    same = lax.broadcasted_iota(jnp.int32, (ids_ref.shape[0],) * 2, 0)
    same = same == lax.broadcasted_iota(jnp.int32, same.shape, 1)
    ids = lax.dot_general(
        ids_ref[...].astype(F32).astype(BF16),
        jnp.where(same, 1.0, 0.0).astype(BF16),
        (((0,), (0,)), ((), ())),
        preferred_element_type=F32,
    )
    lane = lax.broadcasted_iota(jnp.int32, (toks, LANES), 1)
    block = jnp.where(lane < ny * nz, (lane % ny) * nz + lane // ny, -1).astype(F32)
    named = jnp.zeros((toks, LANES), F32)
    for k in range(ids.shape[1]):
        named = jnp.where(ids[:, k : k + 1] == block, 1.0, named)
    row = lax.broadcasted_iota(jnp.int32, (toks, toks), 0)
    col = lax.broadcasted_iota(jnp.int32, (toks, toks), 1)
    before = jnp.where(col < row, 1.0, 0.0).astype(BF16)
    position = jnp.dot(before, named.astype(BF16), preferred_element_type=F32)
    slots = jnp.where(named > 0.0, position, -1.0).astype(BF16)
    base = width + LANES
    for k in range(ny):
        out_ref[k, :, width:base] = slots
    for k in range(ny):
        copies[k].wait()
        for g in range(part // toks):
            out_ref[k, :, base + g * LANES : base + (g + 1) * LANES] = in_rows[
                k, g * toks : (g + 1) * toks, :
            ]
    for c in copies[ny:]:
        c.wait()


def pack(tokens, ids, w_in, dims):
    ny, _, _, nx, nc = dims
    toks, model = tokens.shape
    width = model // ny
    return pl.pallas_call(
        functools.partial(pack_kernel, dims=dims),
        out_shape=pltpu.VMEM((ny, toks, 2 * width + LANES), BF16),
        in_specs=[HBM, VMEM, HBM],
        out_specs=VMEM,
        scratch_shapes=[
            pltpu.VMEM((ny, width // (nx * nc), LANES), BF16),
            pltpu.SemaphoreType.DMA((2, ny)),
        ],
        name="pack",
    )(tokens, ids, w_in)


def share_kernel(w_ref, out_ref, rows, sem, *, dims):
    ny, _, _, _, nc = dims
    width = out_ref.shape[2]
    part = lax.axis_index("x") * nc + lax.axis_index("c")
    top = pl.ds(pl.multiple_of(part * rows.shape[0], 16), rows.shape[0])
    load = pltpu.make_async_copy(w_ref.at[top, :], rows, sem)
    load.start()
    load.wait()
    for k in range(ny):
        out_ref[k] = rows[:, k * width : (k + 1) * width]


def share(w, dims):
    ny, _, _, nx, nc = dims
    rows = w.shape[0] // (nx * nc)
    return pl.pallas_call(
        functools.partial(share_kernel, dims=dims),
        out_shape=jax.ShapeDtypeStruct((ny, rows, w.shape[1] // ny), BF16),
        in_specs=[HBM],
        out_specs=VMEM,
        scratch_shapes=[pltpu.VMEM((rows, w.shape[1]), BF16), pltpu.SemaphoreType.DMA],
        name="share",
    )(w)


def join_kernel(mine_ref, other_ref, out_ref):
    for k in range(mine_ref.shape[0]):
        out_ref[k, 0] = mine_ref[k]
        out_ref[k, 1] = other_ref[k]


def join(mine, other):
    return pl.pallas_call(
        join_kernel,
        out_shape=jax.ShapeDtypeStruct((mine.shape[0], 2) + mine.shape[1:], BF16),
        in_specs=[VMEM, VMEM],
        out_specs=VMEM,
        name="join",
    )(mine, other)


def tile_kernel(mine_ref, other_ref, wide_ref, *, dims):
    ny, _, _, nx, nc = dims
    x, c = lax.axis_index("x"), lax.axis_index("c")
    rows, width = mine_ref.shape[2:]
    groups = width // LANES
    for source, core in ((mine_ref, c), (other_ref, nc - 1 - c)):
        for s in range(nx):
            share = (x + nx - s) % nx * nc + core
            for g in range(groups):
                top = pl.multiple_of((share * groups + g) * rows, 16)
                for k in range(ny):
                    wide_ref[pl.ds(top, rows), k * LANES : (k + 1) * LANES] = source[
                        s, k, :, g * LANES : (g + 1) * LANES
                    ]


def tile(mine, other, dims):
    ny, width = dims[0], mine.shape[3]
    return pl.pallas_call(
        functools.partial(tile_kernel, dims=dims),
        out_shape=pltpu.VMEM((width, ny * LANES), BF16),
        in_specs=[VMEM, VMEM],
        out_specs=VMEM,
        compiler_params=room(56),
        name="tile",
    )(mine, other)


def first_kernel(x_ref, wide_ref, out_ref, bands, sems, *, dims, toks):
    ny, nn, nm, _, _ = dims
    width = wide_ref.shape[0]
    band = ny * toks
    order = [a * nm + m for m in range(nm) for a in range(nn)]
    copies = {
        r: pltpu.make_async_copy(x_ref.at[pl.ds(r * band, band), :], bands.at[r], sems.at[r])
        for r in order
    }
    for r in order:
        copies[r].start()
    per = CHUNK // toks * CAP
    base = (lax.axis_index("zn") * nm + lax.axis_index("zm")) * ny
    row = lax.broadcasted_iota(jnp.int32, (16, LANES), 0)
    lane = lax.broadcasted_iota(jnp.int32, (16, LANES), 1)
    pick = jnp.where((lane == base + row) & (row < ny), 1.0, 0.0).astype(BF16)
    col = lax.broadcasted_iota(jnp.int32, (16, CHUNK), 1)
    slot = lax.broadcasted_iota(jnp.int32, (per, CHUNK), 0).astype(F32)
    first = (col // toks * CAP).astype(F32)
    step = CHUNK // band
    for m in range(len(order) // step):
        used = order[m * step : (m + 1) * step]
        for r in used:
            copies[r].wait()
        x = jnp.concatenate([bands[r] for r in used], axis=0)
        h = jnp.dot(x[:, 0:width], wide_ref[...], preferred_element_type=F32).astype(BF16)
        at = lax.dot_general(
            pick, x[:, width : width + LANES], (((1,), (1,)), ((), ())), preferred_element_type=F32
        )
        at = jnp.where(at >= 0.0, at + first, -1.0)
        for j in range(ny):
            s = jnp.where(slot == at[j : j + 1, :], 1.0, 0.0).astype(BF16)
            rows_j = jnp.dot(s, h[:, j * LANES : (j + 1) * LANES], preferred_element_type=F32)
            out_ref[j, m * per : (m + 1) * per, :] = rows_j.astype(BF16)


def first_product(x, wide, dims, toks):
    ny, nn, nm, _, _ = dims
    slots = x.shape[0] // toks * CAP
    return pl.pallas_call(
        functools.partial(first_kernel, dims=dims, toks=toks),
        out_shape=pltpu.VMEM((ny, slots, LANES), BF16),
        in_specs=[HBM, VMEM],
        out_specs=VMEM,
        scratch_shapes=[
            pltpu.VMEM((nn * nm, ny * toks, x.shape[1]), BF16),
            pltpu.SemaphoreType.DMA((nn * nm,)),
        ],
        name="first_product",
    )(x, wide)


def activate_kernel(part_ref, bias_ref, out_ref, *, dims):
    ny, _, nm, _, _ = dims
    rows = out_ref.shape[1]
    for m in range(nm):
        total = part_ref[0, m * rows : (m + 1) * rows, :].astype(F32)
        for k in range(1, ny):
            total = total + part_ref[k, m * rows : (m + 1) * rows, :].astype(F32)
        h = jnp.maximum(total + bias_ref[...], 0.0).astype(BF16)
        for k in range(ny):
            out_ref[k * nm + m] = h


def activate(part, bias, dims):
    ny, _, nm, _, _ = dims
    return pl.pallas_call(
        functools.partial(activate_kernel, dims=dims),
        out_shape=pltpu.VMEM((ny * nm, part.shape[1] // nm, LANES), BF16),
        in_specs=[VMEM, VMEM],
        out_specs=VMEM,
        name="activate",
    )(part, bias)


def place_kernel(x_ref, place_ref, marks, sems, *, dims, toks):
    ny, nn, nm, _, _ = dims
    zn, zm = lax.axis_index("zn"), lax.axis_index("zm")
    width = x_ref.shape[1] - LANES
    blocks = ny * nm
    band = ny * toks
    copies = []
    for a in range(nn):
        top = pl.multiple_of((a * nm + zm) * band, band)
        copies.append(
            pltpu.make_async_copy(
                x_ref.at[pl.ds(top, band), pl.ds(width, LANES)], marks.at[a], sems.at[a]
            )
        )
    for c in copies:
        c.start()
    per = CHUNK // toks * CAP
    row = lax.broadcasted_iota(jnp.int32, (blocks, LANES), 0)
    lane = lax.broadcasted_iota(jnp.int32, (blocks, LANES), 1)
    pick = jnp.where(lane == (zn * nm + row % nm) * ny + row // nm, 1.0, 0.0).astype(BF16)
    row = lax.broadcasted_iota(jnp.int32, (CHUNK, blocks), 0)
    slot = lax.broadcasted_iota(jnp.int32, (CHUNK, per), 1).astype(F32)
    first = (row // toks * CAP).astype(F32)
    step = CHUNK // band
    for c in copies:
        c.wait()
    for m in range(nn // step):
        at = lax.dot_general(
            jnp.concatenate([marks[m * step + i] for i in range(step)], axis=0),
            pick,
            (((1,), (1,)), ((), ())),
            preferred_element_type=F32,
        )
        at = jnp.where(at >= 0.0, at + first, -1.0)
        for b in range(blocks):
            place_ref[m, b] = jnp.where(slot == at[:, b : b + 1], 1.0, 0.0).astype(BF16)


def place(x, dims, toks):
    ny, nn, nm, _, _ = dims
    band = ny * toks
    return pl.pallas_call(
        functools.partial(place_kernel, dims=dims, toks=toks),
        out_shape=pltpu.VMEM((nn * band // CHUNK, ny * nm, CHUNK, CHUNK // toks * CAP), BF16),
        in_specs=[HBM],
        out_specs=VMEM,
        scratch_shapes=[
            pltpu.VMEM((nn, band, LANES), BF16),
            pltpu.SemaphoreType.DMA((nn,)),
        ],
        name="place",
    )(x)


def second_kernel(h_ref, place_ref, w_ref, out_ref, tall, spread, sems, *, dims, toks):
    chunks, blocks, _, per = place_ref.shape
    width = w_ref.shape[3]
    devices = CHUNK // toks
    nm, zm = dims[2], lax.axis_index("zm")
    copies = []
    for b in range(blocks):
        source = b // nm * nm + (b + nm - zm) % nm
        copies.append(pltpu.make_async_copy(w_ref.at[:, source], tall.at[b], sems.at[b]))
    for c in copies:
        c.start()
    for m in range(chunks):
        for b in range(blocks):
            full = jnp.dot(
                place_ref[m, b], h_ref[b, m * per : (m + 1) * per, :], preferred_element_type=F32
            )
            spread[m, :, b * LANES : (b + 1) * LANES] = full.astype(BF16)
    for c in copies:
        c.wait()
    for m in range(chunks):
        out = jnp.dot(
            spread[m], tall[...].reshape(blocks * LANES, width), preferred_element_type=F32
        )
        out_ref[m * devices : (m + 1) * devices] = out.astype(BF16).reshape(devices, toks, width)


def second_product(h, places, w, dims, toks):
    chunks, blocks = places.shape[:2]
    nt, _, rows, width = w.shape
    return pl.pallas_call(
        functools.partial(second_kernel, dims=dims, toks=toks),
        out_shape=pltpu.VMEM((chunks * CHUNK // toks, toks, width), BF16),
        in_specs=[VMEM, VMEM, HBM],
        out_specs=VMEM,
        scratch_shapes=[
            pltpu.VMEM((blocks, nt, rows, width), BF16),
            pltpu.VMEM((chunks, CHUNK, blocks * LANES), BF16),
            pltpu.SemaphoreType.DMA((blocks,)),
        ],
        compiler_params=room(58),
        name="second_product",
    )(h, places, w)


def combine_kernel(y_ref, out_ref, *, ny):
    width = y_ref.shape[2]
    for k in range(ny):
        total = y_ref[k].astype(F32)
        for other in range(ny + k, y_ref.shape[0], ny):
            total = total + y_ref[other].astype(F32)
        out_ref[:, k * width : (k + 1) * width] = total.astype(BF16)


def combine(y, ny):
    return pl.pallas_call(
        functools.partial(combine_kernel, ny=ny),
        out_shape=jax.ShapeDtypeStruct((y.shape[1], y.shape[2] * ny), BF16),
        in_specs=[VMEM],
        out_specs=VMEM,
        name="combine",
    )(y)


def exchange(value, axes):
    return lax.all_to_all(value, axes, split_axis=0, concat_axis=0, tiled=True)


def body(tokens, block_ids, w_in, bias_in, w_out):
    dims = sizes()
    ny, _, nm, nx, nc = dims
    toks = tokens.shape[0]
    width = tokens.shape[1] // ny

    payload = pack(tokens, block_ids.T, w_in, dims)
    got = exchange(payload, "y")
    w2 = share(w_out, dims)
    pair = lax.ppermute(w2, "zm", [(i, nm - 1 - i) for i in range(nm)])
    w2 = join(near(w2), near(pair))
    x = lax.all_gather(
        got[:, :, : width + LANES].reshape(ny * toks, width + LANES), ("zn", "zm"), axis=0, tiled=True
    )
    w1 = got[:, :, width + LANES :]
    w2 = exchange(w2, "y")
    mine = [w1]
    for s in range(1, nx):
        mine.append(lax.ppermute(w1, "x", [(i, (i + s) % nx) for i in range(nx)]))
    mine = jnp.stack(mine)
    other = lax.ppermute(mine, "c", [(i, nc - 1 - i) for i in range(nc)])
    wide = tile(near(mine), near(other), dims)
    x, wide, w2 = lax.optimization_barrier((x, wide, w2))
    w2 = w2.reshape((1, ny * nm) + w2.shape[2:])
    w2 = lax.all_gather(w2, ("x", "c"), axis=0, tiled=True)

    h = exchange(first_product(x, near(wide), dims, toks), "y")
    h = activate(near(h), bias_in[None, :], dims)
    h = exchange(h, ("y", "zm"))
    places = place(x, dims, toks)
    y = exchange(second_product(near(h), near(places), w2, dims, toks), ("zn", "y"))
    return combine(near(y), ny)


def solution(mesh):
    side = math.isqrt(mesh.shape["blk"])
    cores, pair = 2, 2
    fine = Mesh(
        mesh.devices.reshape(side, side // pair, pair, mesh.shape["tok"] // cores, cores),
        ("y", "zn", "zm", "x", "c"),
    )
    rows = ("x", "c", "y", "zn", "zm")
    blocks = ("y", "zn", "zm")
    return jax.shard_map(
        body,
        mesh=fine,
        in_specs=(P(rows, None), P(rows, None), P(None, blocks), P(blocks), P(blocks, None)),
        out_specs=P(rows, None),
        check_vma=False,
    )
```

```python
import functools
import math

import jax
import jax.numpy as jnp
from jax import lax
from jax.experimental import pallas as pl
from jax.experimental.pallas import tpu as pltpu
from jax.sharding import Mesh
from jax.sharding import PartitionSpec as P


CAP = 5
LANES = 128
CHUNK = 256
BF16 = jnp.bfloat16
F32 = jnp.float32
HBM = pl.BlockSpec(memory_space=pltpu.HBM)
VMEM = pl.BlockSpec(memory_space=pltpu.VMEM)


def sizes():
    ny, nn, nm = lax.axis_size("y"), lax.axis_size("zn"), lax.axis_size("zm")
    return ny, nn, nm, lax.axis_size("x"), lax.axis_size("c")


def room(mebibytes):
    return pltpu.CompilerParams(vmem_limit_bytes=mebibytes << 20)


def near(value):
    return pltpu.with_memory_space_constraint(value, pltpu.VMEM)


def pack_kernel(tokens_ref, ids_ref, w_in_ref, out_ref, id_rows, in_rows, id_sem, sems, *, dims):
    ny, nn, nm, nx, nc = dims
    nz, nt = nn * nm, nx * nc
    share = lax.axis_index("x") * nc + lax.axis_index("c")
    width = tokens_ref.shape[1] // ny
    part = width // nt
    toks = tokens_ref.shape[0]
    copies = []
    for k in range(ny):
        top = pl.multiple_of(k * width + share * part, 16)
        copies.append(
            pltpu.make_async_copy(w_in_ref.at[pl.ds(top, part), :], in_rows.at[k], sems.at[0, k])
        )
    for k in range(ny):
        cut = pl.ds(k * width, width)
        copies.append(
            pltpu.make_async_copy(
                tokens_ref.at[:, cut], out_ref.at[k, :, pl.ds(0, width)], sems.at[1, k]
            )
        )
    names = pltpu.make_async_copy(ids_ref, id_rows, id_sem)
    names.start()
    for c in copies:
        c.start()
    names.wait()
    same = lax.broadcasted_iota(jnp.int32, (ids_ref.shape[0],) * 2, 0)
    same = same == lax.broadcasted_iota(jnp.int32, same.shape, 1)
    ids = lax.dot_general(
        id_rows[...].astype(F32).astype(BF16),
        jnp.where(same, 1.0, 0.0).astype(BF16),
        (((0,), (0,)), ((), ())),
        preferred_element_type=F32,
    )
    lane = lax.broadcasted_iota(jnp.int32, (toks, LANES), 1)
    block = jnp.where(lane < ny * nz, (lane % ny) * nz + lane // ny, -1).astype(F32)
    named = jnp.zeros((toks, LANES), F32)
    for k in range(ids.shape[1]):
        named = jnp.where(ids[:, k : k + 1] == block, 1.0, named)
    row = lax.broadcasted_iota(jnp.int32, (toks, toks), 0)
    col = lax.broadcasted_iota(jnp.int32, (toks, toks), 1)
    before = jnp.where(col < row, 1.0, 0.0).astype(BF16)
    position = jnp.dot(before, named.astype(BF16), preferred_element_type=F32)
    slots = jnp.where(named > 0.0, position, -1.0).astype(BF16)
    base = width + LANES
    for k in range(ny):
        out_ref[k, :, width:base] = slots
    for k in range(ny):
        copies[k].wait()
        for g in range(part // toks):
            out_ref[k, :, base + g * LANES : base + (g + 1) * LANES] = in_rows[
                k, g * toks : (g + 1) * toks, :
            ]
    for c in copies[ny:]:
        c.wait()


def pack(tokens, ids, w_in, dims):
    ny, _, _, nx, nc = dims
    toks, model = tokens.shape
    width = model // ny
    return pl.pallas_call(
        functools.partial(pack_kernel, dims=dims),
        out_shape=pltpu.VMEM((ny, toks, 2 * width + LANES), BF16),
        in_specs=[HBM, HBM, HBM],
        out_specs=VMEM,
        scratch_shapes=[
            pltpu.VMEM(ids.shape, ids.dtype),
            pltpu.VMEM((ny, width // (nx * nc), LANES), BF16),
            pltpu.SemaphoreType.DMA,
            pltpu.SemaphoreType.DMA((2, ny)),
        ],
        name="pack",
    )(tokens, ids, w_in)


def share_kernel(w_ref, out_ref, rows, sem, *, dims):
    ny, _, _, _, nc = dims
    width = out_ref.shape[2]
    part = lax.axis_index("x") * nc + lax.axis_index("c")
    top = pl.ds(pl.multiple_of(part * rows.shape[0], 16), rows.shape[0])
    load = pltpu.make_async_copy(w_ref.at[top, :], rows, sem)
    load.start()
    load.wait()
    for k in range(ny):
        out_ref[k] = rows[:, k * width : (k + 1) * width]


def share(w, dims):
    ny, _, _, nx, nc = dims
    rows = w.shape[0] // (nx * nc)
    return pl.pallas_call(
        functools.partial(share_kernel, dims=dims),
        out_shape=jax.ShapeDtypeStruct((ny, rows, w.shape[1] // ny), BF16),
        in_specs=[HBM],
        out_specs=VMEM,
        scratch_shapes=[pltpu.VMEM((rows, w.shape[1]), BF16), pltpu.SemaphoreType.DMA],
        name="share",
    )(w)


def join_kernel(mine_ref, other_ref, out_ref):
    for k in range(mine_ref.shape[0]):
        out_ref[k, 0] = mine_ref[k]
        out_ref[k, 1] = other_ref[k]


def join(mine, other):
    return pl.pallas_call(
        join_kernel,
        out_shape=jax.ShapeDtypeStruct((mine.shape[0], 2) + mine.shape[1:], BF16),
        in_specs=[VMEM, VMEM],
        out_specs=VMEM,
        name="join",
    )(mine, other)


def tile_kernel(mine_ref, other_ref, wide_ref, *, dims):
    ny, _, _, nx, nc = dims
    x, c = lax.axis_index("x"), lax.axis_index("c")
    rows, width = mine_ref.shape[2:]
    groups = width // LANES
    for source, core in ((mine_ref, c), (other_ref, nc - 1 - c)):
        for s in range(nx):
            share = (x + nx - s) % nx * nc + core
            for g in range(groups):
                top = pl.multiple_of((share * groups + g) * rows, 16)
                for k in range(ny):
                    wide_ref[pl.ds(top, rows), k * LANES : (k + 1) * LANES] = source[
                        s, k, :, g * LANES : (g + 1) * LANES
                    ]


def tile(mine, other, dims):
    ny, width = dims[0], mine.shape[3]
    return pl.pallas_call(
        functools.partial(tile_kernel, dims=dims),
        out_shape=pltpu.VMEM((width, ny * LANES), BF16),
        in_specs=[VMEM, VMEM],
        out_specs=VMEM,
        compiler_params=room(56),
        name="tile",
    )(mine, other)


def first_kernel(x_ref, wide_ref, out_ref, bands, sems, *, dims, toks):
    ny, nn, nm, _, _ = dims
    width = wide_ref.shape[0]
    band = ny * toks
    order = [a * nm + m for m in range(nm) for a in range(nn)]
    copies = {
        r: pltpu.make_async_copy(x_ref.at[pl.ds(r * band, band), :], bands.at[r], sems.at[r])
        for r in order
    }
    for r in order:
        copies[r].start()
    per = CHUNK // toks * CAP
    base = (lax.axis_index("zn") * nm + lax.axis_index("zm")) * ny
    row = lax.broadcasted_iota(jnp.int32, (16, LANES), 0)
    lane = lax.broadcasted_iota(jnp.int32, (16, LANES), 1)
    pick = jnp.where((lane == base + row) & (row < ny), 1.0, 0.0).astype(BF16)
    col = lax.broadcasted_iota(jnp.int32, (16, CHUNK), 1)
    slot = lax.broadcasted_iota(jnp.int32, (per, CHUNK), 0).astype(F32)
    first = (col // toks * CAP).astype(F32)
    step = CHUNK // band
    for m in range(len(order) // step):
        used = order[m * step : (m + 1) * step]
        for r in used:
            copies[r].wait()
        x = jnp.concatenate([bands[r] for r in used], axis=0)
        h = jnp.dot(x[:, 0:width], wide_ref[...], preferred_element_type=F32).astype(BF16)
        at = lax.dot_general(
            pick, x[:, width : width + LANES], (((1,), (1,)), ((), ())), preferred_element_type=F32
        )
        at = jnp.where(at >= 0.0, at + first, -1.0)
        for j in range(ny):
            s = jnp.where(slot == at[j : j + 1, :], 1.0, 0.0).astype(BF16)
            rows_j = jnp.dot(s, h[:, j * LANES : (j + 1) * LANES], preferred_element_type=F32)
            out_ref[j, m * per : (m + 1) * per, :] = rows_j.astype(BF16)


def first_product(x, wide, dims, toks):
    ny, nn, nm, _, _ = dims
    slots = x.shape[0] // toks * CAP
    return pl.pallas_call(
        functools.partial(first_kernel, dims=dims, toks=toks),
        out_shape=pltpu.VMEM((ny, slots, LANES), BF16),
        in_specs=[HBM, VMEM],
        out_specs=VMEM,
        scratch_shapes=[
            pltpu.VMEM((nn * nm, ny * toks, x.shape[1]), BF16),
            pltpu.SemaphoreType.DMA((nn * nm,)),
        ],
        name="first_product",
    )(x, wide)


def activate_kernel(part_ref, bias_ref, out_ref, *, dims):
    ny, _, nm, _, _ = dims
    rows = out_ref.shape[1]
    for m in range(nm):
        total = part_ref[0, m * rows : (m + 1) * rows, :].astype(F32)
        for k in range(1, ny):
            total = total + part_ref[k, m * rows : (m + 1) * rows, :].astype(F32)
        h = jnp.maximum(total + bias_ref[...], 0.0).astype(BF16)
        for k in range(ny):
            out_ref[k * nm + m] = h


def activate(part, bias, dims):
    ny, _, nm, _, _ = dims
    return pl.pallas_call(
        functools.partial(activate_kernel, dims=dims),
        out_shape=pltpu.VMEM((ny * nm, part.shape[1] // nm, LANES), BF16),
        in_specs=[VMEM, VMEM],
        out_specs=VMEM,
        name="activate",
    )(part, bias)


def place_kernel(x_ref, place_ref, marks, sems, *, dims, toks):
    ny, nn, nm, _, _ = dims
    zn, zm = lax.axis_index("zn"), lax.axis_index("zm")
    width = x_ref.shape[1] - LANES
    blocks = ny * nm
    band = ny * toks
    copies = []
    for a in range(nn):
        top = pl.multiple_of((a * nm + zm) * band, band)
        copies.append(
            pltpu.make_async_copy(
                x_ref.at[pl.ds(top, band), pl.ds(width, LANES)], marks.at[a], sems.at[a]
            )
        )
    for c in copies:
        c.start()
    per = CHUNK // toks * CAP
    row = lax.broadcasted_iota(jnp.int32, (blocks, LANES), 0)
    lane = lax.broadcasted_iota(jnp.int32, (blocks, LANES), 1)
    pick = jnp.where(lane == (zn * nm + row % nm) * ny + row // nm, 1.0, 0.0).astype(BF16)
    row = lax.broadcasted_iota(jnp.int32, (CHUNK, blocks), 0)
    slot = lax.broadcasted_iota(jnp.int32, (CHUNK, per), 1).astype(F32)
    first = (row // toks * CAP).astype(F32)
    step = CHUNK // band
    for c in copies:
        c.wait()
    for m in range(nn // step):
        at = lax.dot_general(
            jnp.concatenate([marks[m * step + i] for i in range(step)], axis=0),
            pick,
            (((1,), (1,)), ((), ())),
            preferred_element_type=F32,
        )
        at = jnp.where(at >= 0.0, at + first, -1.0)
        for b in range(blocks):
            place_ref[m, b] = jnp.where(slot == at[:, b : b + 1], 1.0, 0.0).astype(BF16)


def place(x, dims, toks):
    ny, nn, nm, _, _ = dims
    band = ny * toks
    return pl.pallas_call(
        functools.partial(place_kernel, dims=dims, toks=toks),
        out_shape=pltpu.VMEM((nn * band // CHUNK, ny * nm, CHUNK, CHUNK // toks * CAP), BF16),
        in_specs=[HBM],
        out_specs=VMEM,
        scratch_shapes=[
            pltpu.VMEM((nn, band, LANES), BF16),
            pltpu.SemaphoreType.DMA((nn,)),
        ],
        name="place",
    )(x)


def second_kernel(h_ref, place_ref, w_ref, out_ref, tall, spread, sems, *, dims, toks):
    chunks, blocks, _, per = place_ref.shape
    width = w_ref.shape[3]
    devices = CHUNK // toks
    nm, zm = dims[2], lax.axis_index("zm")
    copies = []
    for b in range(blocks):
        source = b // nm * nm + (b + nm - zm) % nm
        copies.append(pltpu.make_async_copy(w_ref.at[:, source], tall.at[b], sems.at[b]))
    for c in copies:
        c.start()
    for m in range(chunks):
        for b in range(blocks):
            full = jnp.dot(
                place_ref[m, b], h_ref[b, m * per : (m + 1) * per, :], preferred_element_type=F32
            )
            spread[m, :, b * LANES : (b + 1) * LANES] = full.astype(BF16)
        if m == 0:
            for c in copies:
                c.wait()
        out = jnp.dot(
            spread[m], tall[...].reshape(blocks * LANES, width), preferred_element_type=F32
        )
        out_ref[m * devices : (m + 1) * devices] = out.astype(BF16).reshape(devices, toks, width)


def second_product(h, places, w, dims, toks):
    chunks, blocks = places.shape[:2]
    nt, _, rows, width = w.shape
    return pl.pallas_call(
        functools.partial(second_kernel, dims=dims, toks=toks),
        out_shape=pltpu.VMEM((chunks * CHUNK // toks, toks, width), BF16),
        in_specs=[VMEM, VMEM, HBM],
        out_specs=VMEM,
        scratch_shapes=[
            pltpu.VMEM((blocks, nt, rows, width), BF16),
            pltpu.VMEM((chunks, CHUNK, blocks * LANES), BF16),
            pltpu.SemaphoreType.DMA((blocks,)),
        ],
        compiler_params=room(58),
        name="second_product",
    )(h, places, w)


def combine_kernel(y_ref, out_ref, *, ny):
    width = y_ref.shape[2]
    for k in range(ny):
        total = y_ref[k].astype(F32)
        for other in range(ny + k, y_ref.shape[0], ny):
            total = total + y_ref[other].astype(F32)
        out_ref[:, k * width : (k + 1) * width] = total.astype(BF16)


def combine(y, ny):
    return pl.pallas_call(
        functools.partial(combine_kernel, ny=ny),
        out_shape=jax.ShapeDtypeStruct((y.shape[1], y.shape[2] * ny), BF16),
        in_specs=[VMEM],
        out_specs=VMEM,
        name="combine",
    )(y)


def exchange(value, axes):
    return lax.all_to_all(value, axes, split_axis=0, concat_axis=0, tiled=True)


def body(tokens, block_ids, w_in, bias_in, w_out):
    dims = sizes()
    ny, _, nm, nx, nc = dims
    toks = tokens.shape[0]
    width = tokens.shape[1] // ny

    payload = pack(tokens, block_ids.T, w_in, dims)
    got = exchange(payload, "y")
    w2 = share(w_out, dims)
    pair = lax.ppermute(w2, "zm", [(i, nm - 1 - i) for i in range(nm)])
    w2 = join(near(w2), near(pair))
    x = lax.all_gather(
        got[:, :, : width + LANES].reshape(ny * toks, width + LANES), ("zn", "zm"), axis=0, tiled=True
    )
    w1 = got[:, :, width + LANES :]
    w2 = exchange(w2, "y")
    mine = [w1]
    for s in range(1, nx):
        mine.append(lax.ppermute(w1, "x", [(i, (i + s) % nx) for i in range(nx)]))
    mine = jnp.stack(mine)
    other = lax.ppermute(mine, "c", [(i, nc - 1 - i) for i in range(nc)])
    wide = tile(near(mine), near(other), dims)
    x, wide, w2 = lax.optimization_barrier((x, wide, w2))
    w2 = w2.reshape((1, ny * nm) + w2.shape[2:])
    w2 = lax.all_gather(w2, ("x", "c"), axis=0, tiled=True)

    h = exchange(first_product(x, near(wide), dims, toks), "y")
    h = activate(near(h), near(bias_in[None, :]), dims)
    h = exchange(h, ("y", "zm"))
    places = place(x, dims, toks)
    y = exchange(second_product(near(h), near(places), w2, dims, toks), ("zn", "y"))
    return combine(near(y), ny)


def solution(mesh):
    side = math.isqrt(mesh.shape["blk"])
    cores, pair = 2, 2
    fine = Mesh(
        mesh.devices.reshape(side, side // pair, pair, mesh.shape["tok"] // cores, cores),
        ("y", "zn", "zm", "x", "c"),
    )
    rows = ("x", "c", "y", "zn", "zm")
    blocks = ("y", "zn", "zm")
    return jax.shard_map(
        body,
        mesh=fine,
        in_specs=(P(rows, None), P(rows, None), P(None, blocks), P(blocks), P(blocks, None)),
        out_specs=P(rows, None),
        check_vma=False,
    )
```
